32 devices in a mesh: depth: 2 (over core), tile: 16 (over z, y, x).
Axes of the slice: x: 2, y: 2, z: 4, core: 2. Of those that a mesh axis runs over, the one named last changes fastest.
Arguments:
- volume: float32 [8, 512, 1024], P('depth', 'tile'), may hold values from -6 to 6
- measured: float32 [3, 512, 1024], P(None, 'tile'), may hold values from -12 to 12
- row_bank: float32 [256, 2, 33], replicated, may hold values from -1 to 1
- col_bank: float32 [256, 2, 33], replicated, may hold values from -1 to 1
- kernel_index: int32 [169, 8], P(None, 'depth'), may hold values from 0 to 255
- view_order: int32 [3], replicated, may hold values from 0 to 168
Outputs:
- volume_out: float32 [8, 512, 1024], P('depth', 'tile')
- last_residual: float32 [512, 1024], P('tile')
The draws below stay inside these ranges and needn't reach their ends.
All inputs are finite; a program needn't handle non-finite values.
Results may differ from the reference program's by a relative error of at most 0.00013.
Values sent between devices are 32-bit elements; how exact they have to be, the bound alone decides.
No kernel may reach another device: no remote copies, remote signals or barrier semaphores. Data moves between devices by JAX's collectives and lax.ppermute only.
A program may use at most 64 MiB of HBM per device.

```python
import jax
import jax.numpy as jnp
from jax import lax

WIDTH = 1024
TAPS = 33
BANK = 256
VIEWS = 169
NV = 3
DEPTH = 8
HEIGHT = 512


def with_ends(result, key, smallest, largest):
    longest = result.shape.index(max(result.shape))
    spots = []
    for shift in (0, 1):
        where = [jax.random.randint(jax.random.fold_in(key, axis), (), 0, length) for axis, length in enumerate(result.shape)]
        where[longest] = (where[longest] + shift) % result.shape[longest]
        spots.append(tuple(where))
    return result.at[spots[0]].set(smallest).at[spots[1]].set(largest)


def block_scale(rng, extent, shards, smallest, largest):
    gain, own = 1.0, jax.random.fold_in(rng, 6)
    for dim, blocks in shards:
        heights = jnp.exp(jax.random.uniform(jax.random.fold_in(own, dim), (blocks,), jnp.float32, smallest / len(shards), largest / len(shards)))
        gain = gain * jnp.repeat(heights, extent[dim] // blocks).reshape([-1 if axis == dim else 1 for axis in range(len(extent))])
    return gain


def normal_values(stream_key, dims, scale, most, split=(), kind=jnp.bfloat16):
    array = jax.random.normal(stream_key, dims, jnp.float32) * scale
    if len(split) > 0:
        array = block_scale(stream_key, dims, split, -0.22, 0.18) * array
    return jnp.clip(array, min=-most, max=most).astype(kind)


def setup_inputs(seed: int = 0) -> dict:
    streams_of = jax.random.split(jax.random.key(seed), 7)
    volume = normal_values(streams_of[0], (DEPTH, HEIGHT, WIDTH), 1.0, 6.0, ((0, 2), (1, 16)), jnp.float32)
    measured = normal_values(streams_of[1], (NV, HEIGHT, WIDTH), 2.0, 12.0, ((1, 16),), jnp.float32)
    row_bank = normal_values(streams_of[2], (BANK, 2, TAPS), (33 * 2 * DEPTH // 14) ** -0.5, 1.0, (), jnp.float32)
    col_bank = normal_values(streams_of[3], (BANK, 2, TAPS), (33 * 2 * DEPTH // 14) ** -0.5, 1.0, (), jnp.float32)
    kernel_index = with_ends(jax.random.randint(streams_of[4], (VIEWS, DEPTH), 0, BANK), jax.random.fold_in(streams_of[4], 1), 0, BANK - 1).astype(jnp.int32)
    view_order = jax.random.randint(streams_of[5], (NV,), 0, VIEWS).astype(jnp.int32)
    return dict(volume=volume, measured=measured, row_bank=row_bank, col_bank=col_bank, kernel_index=kernel_index, view_order=view_order)


descent_step = 0.5
shrinkage = 0.1


def row_pass(extended, taps, rows):
    total = taps[:, :, 0, None, None] * extended[:, :, 0:rows, :]
    for shift_k in range(1, taps.shape[2]):
        total = total + taps[:, :, shift_k, None, None] * extended[:, :, shift_k:shift_k + rows, :]
    return total


def col_pass(upper, taps):
    width = upper.shape[3]
    reach = (taps.shape[2] - 1) // 2
    padded = jnp.pad(upper, ((0, 0), (0, 0), (0, 0), (reach, reach)))
    total = taps[:, :, 0, None, None] * padded[:, :, :, 0:width]
    for shift_k in range(1, taps.shape[2]):
        total = total + taps[:, :, shift_k, None, None] * padded[:, :, :, shift_k:shift_k + width]
    return total


def reference(volume, measured, row_bank, col_bank, kernel_index, view_order):
    reach = (row_bank.shape[2] - 1) // 2
    height = volume.shape[1]
    width = volume.shape[2]
    residual = jnp.zeros((height, width), jnp.float32)
    for step in range(measured.shape[0]):
        entries = kernel_index[view_order[step]]
        row_taps = jnp.take(row_bank, entries, axis=0)
        col_taps = jnp.take(col_bank, entries, axis=0)

        def add_plane(total, items):
            plane, row_one, col_one = items
            extended = jnp.pad(plane, ((reach, reach), (0, 0)))
            upper = row_pass(extended[None, None], row_one[None], height)
            return total + jnp.sum(col_pass(upper, col_one[None]), axis=(0, 1)), None

        image, _ = lax.scan(add_plane, jnp.zeros((height, width), jnp.float32), (volume, row_taps, col_taps))
        residual = image - measured[step]
        res_ext = jnp.pad(residual, ((reach, reach), (0, 0)))

        def update(items):
            plane, row_one, col_one = items
            upper = row_pass(res_ext[None, None], row_one[None, :, ::-1], height)
            grad = jnp.sum(col_pass(upper, col_one[None, :, ::-1]), axis=(0, 1))
            moved = plane - descent_step * grad
            return moved - jnp.clip(moved, -shrinkage, shrinkage)

        volume = lax.map(update, (volume, row_taps, col_taps))
    return volume, residual
```

```python
import functools

import jax
import jax.numpy as jnp
from jax import lax
from jax.experimental import pallas as pl
from jax.experimental.pallas import tpu as pltpu
from jax.sharding import PartitionSpec as P

descent_step = 0.5
shrinkage = 0.1
LANES = 128
HALF = LANES // 2
bf16, f32 = jnp.bfloat16, jnp.float32


def split(x):
    hi = x.astype(bf16)
    return hi, (x - hi.astype(f32)).astype(bf16)


def dot(a, b):
    return lax.dot_general(a, b, (((1,), (0,)), ((), ())), preferred_element_type=f32)


def dot_nt(a, b):
    return lax.dot_general(a, b, (((1,), (1,)), ((), ())), preferred_element_type=f32)


def lane_iota(shape):
    return lax.broadcasted_iota(jnp.int32, shape, 1)


def row_iota(shape):
    return lax.broadcasted_iota(jnp.int32, shape, 0)


def tap_rows(bank_ref, entry):
    taps = bank_ref[entry]
    pad = jnp.zeros((taps.shape[0], LANES - taps.shape[1]), f32)
    return jnp.concatenate([taps, pad], axis=1)


def prepare(steps, spots, view_ref, index_ref, place_ref, row_bank, col_bank, outs):
    fwd_hi, fwd_lo, adj, row_hi, row_lo, adj_rows = outs
    planes = index_ref.shape[1]
    reach = (row_bank.shape[2] - 1) // 2
    rows = 2 * reach
    flag, first, last = place_ref[0], place_ref[1], place_ref[2]
    square = (LANES, LANES)
    below = lane_iota(square) < row_iota(square)
    above = lane_iota(square) > row_iota(square)
    per_lane = LANES // rows
    window = row_iota((8, LANES))
    for s, step in zip(spots, steps):
        view = view_ref[step]
        row_parts = []
        for d in range(planes):
            entry = index_ref[view, d]
            col = tap_rows(col_bank, entry)
            row = tap_rows(row_bank, entry)
            for r in range(2):
                base = pltpu.roll(
                    jnp.broadcast_to(col[r : r + 1], (8, LANES)),
                    (LANES - HALF - reach) % LANES, 1, stride=1, stride_axis=0,
                )
                ring = jnp.concatenate(
                    [base] + [pltpu.roll(base, 8 * b, 1) for b in range(1, LANES // 8)], axis=0
                )
                hi, lo = split(ring)
                hi, lo = hi.astype(f32), lo.astype(f32)
                low_hi = jnp.where(below, hi, 0.0).astype(bf16)
                low_lo = jnp.where(below, lo, 0.0).astype(bf16)
                up_hi = jnp.where(above, hi, 0.0).astype(bf16)
                up_lo = jnp.where(above, lo, 0.0).astype(bf16)
                here = pl.ds(r * LANES, LANES)
                fwd_hi[s, d, here, 0:LANES] = up_hi
                fwd_hi[s, d, here, LANES : 2 * LANES] = low_hi
                fwd_lo[s, d, here, 0:LANES] = up_lo
                fwd_lo[s, d, here, LANES : 2 * LANES] = low_lo
                adj[s, d, r, 0:LANES, 0:LANES] = low_hi
                adj[s, d, r, 0:LANES, LANES : 2 * LANES] = low_lo
                adj[s, d, r, LANES : 2 * LANES, 0:LANES] = up_hi
                adj[s, d, r, LANES : 2 * LANES, LANES : 2 * LANES] = up_lo
                spot = ((2 * d + r) % per_lane) * rows
                row_parts.append(
                    pltpu.roll(
                        jnp.broadcast_to(row[r : r + 1], (8, LANES)),
                        (spot - 2 * reach) % LANES, 1, stride=1, stride_axis=0,
                    )
                )
        bands = []
        lane = lane_iota((8, LANES)) // rows
        for band in range(2 * rows // 8):
            upper = band < rows // 8
            start = (8 * band) % rows
            offset = start + rows * (flag if upper else 1 - flag)
            line = window + offset
            good = jnp.logical_and(
                jnp.logical_or(first == 0, line >= reach),
                jnp.logical_or(last == 0, line < rows + reach),
            )
            groups = []
            for group in range(2 * planes // per_lane):
                total = jnp.zeros((8, LANES), f32)
                for k in range(per_lane):
                    part = pltpu.roll(row_parts[group * per_lane + k], offset, 1)
                    total = jnp.where(lane == k, part, total)
                groups.append(jnp.where(good, total, 0.0))
            bands.append(jnp.concatenate(groups, axis=1))
        stack = jnp.concatenate(bands, axis=0)
        hi, lo = split(stack)
        row_hi[s] = hi
        row_lo[s] = lo
        turned = stack.T
        hi, lo = split(turned)
        adj_rows[s] = jnp.concatenate([hi, hi, lo], axis=1)


def forward(volume, fwd_hi, fwd_lo, row_hi, row_lo, target, w_hi, w_lo):
    planes = len(volume)
    rows, width = volume[0].shape
    blocks = width // LANES
    zero = jnp.zeros((rows, LANES), bf16)
    left = lane_iota((rows, LANES)) < HALF
    for d in range(planes):
        sides = []
        for part in split(volume[d]):
            column = [zero] + [part[:, b * LANES : (b + 1) * LANES] for b in range(blocks)] + [zero]
            column = jnp.concatenate(column, axis=0)
            sides.append(jnp.concatenate([column[: -rows], column[rows:]], axis=1))
        hi, lo = sides
        wide = dot_nt(hi, fwd_hi[d]) + dot_nt(lo, fwd_hi[d]) + dot_nt(hi, fwd_lo[d])
        for r in range(2):
            part = wide[:, r * LANES : (r + 1) * LANES]
            spot = pl.ds((2 * d + r) * rows, rows)
            for c in range(blocks):
                block = part[c * rows : (c + 1) * rows]
                if c == 0:
                    block = jnp.where(left, part[blocks * rows :], block)
                hi_w, lo_w = split(block)
                w_hi[spot, c * LANES : (c + 1) * LANES] = hi_w
                w_lo[spot, c * LANES : (c + 1) * LANES] = lo_w
    image = (
        dot(row_hi, w_hi[...]) + dot(row_lo, w_hi[...]) + dot(row_hi, w_lo[...])
    )
    return image[:rows] - target, image[rows:]


def adjoint(residual, adj_rows, adj, volume):
    planes = len(volume)
    rows, width = volume[0].shape
    blocks = width // LANES
    hi, lo = split(residual)
    upper = dot(adj_rows, jnp.concatenate([hi, lo, hi], axis=0))
    left = lane_iota((rows, LANES)) < HALF
    result = []
    for d in range(planes):
        total = None
        for r in range(2):
            spot = (2 * d + r) * rows
            part = upper[spot : spot + rows]
            edge = part[:, :LANES]
            column = [jnp.where(left, 0.0, edge)]
            column += [part[:, b * LANES : (b + 1) * LANES] for b in range(1, blocks)]
            column += [jnp.where(left, edge, 0.0)]
            for side in split(jnp.concatenate(column, axis=0)):
                side = jnp.concatenate([side[: -rows], side[rows:]], axis=1)
                term = dot(side, adj[d, r])
                total = term if total is None else total + term
        grad = total[:, :LANES] + total[:, LANES:]
        grad = jnp.concatenate([grad[c * rows : (c + 1) * rows] for c in range(blocks)], axis=1)
        moved = volume[d] - descent_step * grad
        result.append(moved - jnp.clip(moved, -shrinkage, shrinkage))
    return result


def window_target(measured, flag, use):
    reach = measured.shape[0] // 2
    upper = jnp.where(flag == 1, measured[reach:], 0.0)
    lower = jnp.where(flag == 1, 0.0, measured[:reach])
    both = jnp.where(use == 1, jnp.concatenate([upper, lower], axis=0), 0.0)
    return pltpu.roll(both, HALF, 1)


def first_kernel(
    place, view, index, row_bank, col_bank, volume, measured,
    mine, other, adj, adj_rows, fwd_hi, fwd_lo, row_hi, row_lo, w_hi, w_lo,
):
    outs = (fwd_hi, fwd_lo, adj, row_hi, row_lo, adj_rows)
    prepare((0,), (0,), view, index, place, row_bank, col_bank, outs)
    planes = [volume[d] for d in range(volume.shape[0])]
    target = window_target(measured[0], place[0], place[3])
    mine[...], other[...] = forward(
        planes, fwd_hi.at[0], fwd_lo.at[0], row_hi[0], row_lo[0], target, w_hi, w_lo
    )


def prepare_kernel(steps, place, view, index, row_bank, col_bank, *outs):
    prepare(steps, range(len(steps)), view, index, place, row_bank, col_bank, outs)


def middle_kernel(
    step, spot, old, place, s_ref, o_ref, adj, adj_rows, fwd_hi, fwd_lo, row_hi, row_lo,
    volume, measured, mine, other, fresh, w_hi, w_lo,
):
    residual = jnp.concatenate([s_ref[...], o_ref[...]], axis=0)
    planes = [volume[d] for d in range(volume.shape[0])]
    planes = adjoint(residual, adj_rows[old], adj.at[old], planes)
    for d, plane in enumerate(planes):
        fresh[d] = plane
    target = window_target(measured[step], place[0], place[3])
    mine[...], other[...] = forward(
        planes, fwd_hi.at[spot], fwd_lo.at[spot], row_hi[spot], row_lo[spot], target, w_hi, w_lo
    )


def last_kernel(old, place, s_ref, o_ref, adj, adj_rows, volume, fresh, residual_out):
    mine, other = s_ref[...], o_ref[...]
    reach = mine.shape[0] // 2
    flag = place[0] == 1
    own = jnp.concatenate(
        [jnp.where(flag, other[reach:], mine[reach:]), jnp.where(flag, mine[:reach], other[:reach])],
        axis=0,
    )
    residual_out[...] = pltpu.roll(own, own.shape[1] - HALF, 1)
    planes = [volume[d] for d in range(volume.shape[0])]
    planes = adjoint(
        jnp.concatenate([mine, other], axis=0), adj_rows[old], adj.at[old], planes
    )
    for d, plane in enumerate(planes):
        fresh[d] = plane


VMEM = pl.BlockSpec(memory_space=pltpu.VMEM)
SMEM = pl.BlockSpec(memory_space=pltpu.SMEM)


def call(kernel, in_specs, outs, scratch, flops, name, args):
    return pl.pallas_call(
        kernel,
        out_shape=outs,
        in_specs=in_specs,
        out_specs=[VMEM] * len(outs),
        scratch_shapes=scratch,
        compiler_params=pltpu.CompilerParams(vmem_limit_bytes=24 << 20),
        cost_estimate=pl.CostEstimate(flops=flops, bytes_accessed=4 << 20, transcendentals=0),
        name=name,
    )(*args)


def per_device(volume, measured, row_bank, col_bank, kernel_index, view_order):
    planes, rows, width = volume.shape
    steps = measured.shape[0]
    reach = (row_bank.shape[2] - 1) // 2
    assert rows == 2 * reach and width % LANES == 0 and reach <= HALF
    depth, tiles = lax.axis_size("depth"), lax.axis_size("tile")
    d, t = lax.axis_index("depth"), lax.axis_index("tile")
    even = t % 2 == 0
    paired = depth == 2
    lower = (even == (d == 0)) if paired else even
    place = jnp.stack(
        [lower, t == 0, t == tiles - 1, jnp.asarray(paired)]
    ).astype(jnp.int32)

    evens = [(i, i ^ 1) for i in range(tiles) if i ^ 1 < tiles]
    odds = [(i, i + 1 if i % 2 else i - 1) for i in range(tiles)]
    odds = [(i, j) for i, j in odds if 0 <= j < tiles]

    def exchange(mine, other, step):
        if paired:
            swap = [(0, 1), (1, 0)]
            pairs = evens + [(tiles + i, tiles + j) for i, j in odds]
            kept = mine + lax.ppermute(other, "depth", swap)
            kept = kept + lax.ppermute(kept, ("depth", "tile"), pairs)
            return kept, lax.ppermute(kept, "depth", swap)
        target = jnp.roll(measured[step], HALF, axis=1)
        high = jnp.pad(target[:reach], ((reach, 0), (0, 0)))
        low = jnp.pad(target[reach:], ((0, reach), (0, 0)))
        kept = lax.psum(mine, "depth") - jnp.where(lower, low, high)
        rest = lax.psum(other, "depth") - jnp.where(lower, high, low)
        kept = kept + lax.ppermute(kept, "tile", evens)
        rest = rest + lax.ppermute(rest, "tile", odds)
        return kept, rest

    shape = jax.ShapeDtypeStruct
    stacks = 2 * planes * rows

    def operands(n):
        return [
            shape((n, planes, 2 * LANES, 2 * LANES), bf16),
            shape((n, planes, 2 * LANES, 2 * LANES), bf16),
            shape((n, planes, 2, 2 * LANES, 2 * LANES), bf16),
            shape((n, 2 * rows, stacks), bf16),
            shape((n, 2 * rows, stacks), bf16),
            shape((n, stacks, 6 * rows), bf16),
        ]

    image = shape((rows, width), f32)
    wide = [pltpu.VMEM((stacks, width), bf16)] * 2
    flops = 400 << 20
    banks = (place, view_order, kernel_index, row_bank, col_bank)
    bank_specs = [SMEM] * 3 + [VMEM] * 2
    one = operands(1)
    mine, other, adj, adj_rows = call(
        first_kernel, bank_specs + [VMEM] * 2, [image, image, one[2], one[5]],
        [pltpu.VMEM(x.shape, x.dtype) for x in (one[0], one[1], one[3], one[4])] + wide,
        flops, "first", banks + (volume, measured),
    )
    later = tuple(range(1, steps))
    fwd_hi, fwd_lo, adj_later, row_hi, row_lo, adj_rows_later = call(
        functools.partial(prepare_kernel, later), bank_specs, operands(len(later)), [],
        flops, "prepare", banks,
    )
    old = 0
    for step in later:
        kept, rest = exchange(mine, other, step - 1)
        mine, other, volume = call(
            functools.partial(middle_kernel, step, step - 1, old),
            [SMEM] + [VMEM] * 10,
            [image, image, shape(volume.shape, f32)], wide, 2 * flops, "middle",
            (place, kept, rest, adj, adj_rows, fwd_hi, fwd_lo, row_hi, row_lo, volume, measured),
        )
        adj, adj_rows, old = adj_later, adj_rows_later, step - 1
    kept, rest = exchange(mine, other, steps - 1)
    volume, residual = call(
        functools.partial(last_kernel, old), [SMEM] + [VMEM] * 5,
        [shape(volume.shape, f32), image], [], flops, "last",
        (place, kept, rest, adj, adj_rows, volume),
    )
    return volume, residual


def solution(mesh):
    return jax.shard_map(
        per_device,
        mesh=mesh,
        in_specs=(P("depth", "tile", None), P(None, "tile", None), P(), P(), P(None, "depth"), P()),
        out_specs=(P("depth", "tile", None), P("tile", None)),
        check_vma=False,
    )
```

```python
import functools

import jax
import jax.numpy as jnp
from jax import lax
from jax.experimental import pallas as pl
from jax.experimental.pallas import tpu as pltpu
from jax.sharding import PartitionSpec as P

descent_step = 0.5
shrinkage = 0.1
LANES = 128
HALF = LANES // 2
bf16, f32 = jnp.bfloat16, jnp.float32


def split(x):
    hi = x.astype(bf16)
    return hi, (x - hi.astype(f32)).astype(bf16)


def dot(a, b):
    return lax.dot_general(a, b, (((1,), (0,)), ((), ())), preferred_element_type=f32)


def dot_nt(a, b):
    return lax.dot_general(a, b, (((1,), (1,)), ((), ())), preferred_element_type=f32)


def lane_iota(shape):
    return lax.broadcasted_iota(jnp.int32, shape, 1)


def row_iota(shape):
    return lax.broadcasted_iota(jnp.int32, shape, 0)


class Place:
    def __init__(self, paired):
        d, t = lax.axis_index("depth"), lax.axis_index("tile")
        tiles = lax.axis_size("tile")
        odd = lax.rem(t, 2)
        self.first = t == 0
        self.last = t == tiles - 1
        self.flag = 1 - jnp.bitwise_xor(odd, d) if paired else 1 - odd
        end = jnp.logical_and(jnp.logical_or(self.first, self.last), paired)
        self.end_even = jnp.logical_and(end, d == 0)
        self.end_odd = jnp.logical_and(end, d == 1)


def pick_taps(steps, planes, view_ref, index, banks, taps_ref):
    count = taps_ref.shape[1]
    index = index.astype(f32)
    copies = jnp.concatenate([index] * (count // planes), axis=0)
    line, lane = row_iota(copies.shape), lane_iota(copies.shape)
    view = jnp.full(copies.shape, view_ref[0], jnp.int32)
    for step in range(1, steps):
        view = jnp.where(line >= step * planes, view_ref[step], view)
    entry = jnp.sum(jnp.where(lane == view, copies, 0.0), axis=1, keepdims=True)
    size = banks[0].shape[2]
    chosen = (lane_iota((count, size)).astype(f32) == entry).astype(f32).astype(bf16)
    taps_ref[...] = jnp.zeros(taps_ref.shape, f32)
    for b, bank in enumerate(banks):
        for r in range(2):
            hi, lo = split(bank[:, r, :])
            taps = dot_nt(chosen, hi) + dot_nt(chosen, lo)
            taps_ref[2 * b + r, :, 0 : taps.shape[1]] = taps


def column_operands(taps_ref, line, d, reach, forward_out, adjoint_out):
    square = (LANES, LANES)
    below = lane_iota(square) < row_iota(square)
    above = lane_iota(square) > row_iota(square)
    for r in range(2):
        base = pltpu.roll(
            jnp.broadcast_to(taps_ref[2 + r, line : line + 1], (8, LANES)),
            (LANES - HALF - reach) % LANES, 1, stride=1, stride_axis=0,
        )
        ring = jnp.concatenate(
            [base] + [pltpu.roll(base, 8 * b, 1) for b in range(1, LANES // 8)], axis=0
        )
        low_hi, low_lo = split(jnp.where(below, ring, 0.0))
        up_hi, up_lo = split(jnp.where(above, ring, 0.0))
        left, right = slice(0, LANES), slice(LANES, 2 * LANES)
        if forward_out is not None:
            fwd_hi, fwd_lo = forward_out
            here = slice(r * LANES, (r + 1) * LANES)
            fwd_hi[d, here, left] = up_hi
            fwd_hi[d, here, right] = low_hi
            fwd_lo[d, here, left] = up_lo
            fwd_lo[d, here, right] = low_lo
        if adjoint_out is not None:
            adjoint_out[d, r, left, left] = low_hi
            adjoint_out[d, r, left, right] = low_lo
            adjoint_out[d, r, right, left] = up_hi
            adjoint_out[d, r, right, right] = up_lo


def row_operand(taps_ref, step, planes, reach, place):
    rows = 2 * reach
    per_lane = LANES // rows
    window, lane = row_iota((8, LANES)), lane_iota((8, LANES)) // rows
    parts = []
    for k in range(2 * planes):
        line = step * planes + k // 2
        parts.append(
            pltpu.roll(
                jnp.broadcast_to(taps_ref[k % 2, line : line + 1], (8, LANES)),
                ((k % per_lane) * rows - 2 * reach) % LANES, 1, stride=1, stride_axis=0,
            )
        )
    bands = []
    for band in range(2 * rows // 8):
        start = (8 * band) % rows
        offset = start + rows * (place.flag if band < rows // 8 else 1 - place.flag)
        spot = window + offset
        good = jnp.logical_and(
            jnp.logical_or(jnp.logical_not(place.first), spot >= reach),
            jnp.logical_or(jnp.logical_not(place.last), spot < rows + reach),
        )
        line = []
        for group in range(2 * planes // per_lane):
            total = jnp.zeros((8, LANES), f32)
            for k in range(per_lane):
                part = pltpu.roll(parts[group * per_lane + k], offset, 1)
                total = jnp.where(lane == k, part, total)
            line.append(jnp.where(good, total, 0.0))
        bands.append(jnp.concatenate(line, axis=1))
    return jnp.concatenate(bands, axis=0)


def adjoint_row_operand(stack):
    hi, lo = split(stack.T)
    return jnp.concatenate([hi, hi, lo], axis=1)


def forward(volume, fwd_hi, fwd_lo, row_hi, row_lo, target, w_hi, w_lo):
    planes = len(volume)
    rows, width = volume[0].shape
    blocks = width // LANES
    zero = jnp.zeros((rows, LANES), bf16)
    left = lane_iota((rows, LANES)) < HALF
    for d in range(planes):
        sides = []
        for part in split(volume[d]):
            column = [zero] + [part[:, b * LANES : (b + 1) * LANES] for b in range(blocks)] + [zero]
            column = jnp.concatenate(column, axis=0)
            sides.append(jnp.concatenate([column[:-rows], column[rows:]], axis=1))
        hi, lo = sides
        wide = dot_nt(hi, fwd_hi[d]) + dot_nt(lo, fwd_hi[d]) + dot_nt(hi, fwd_lo[d])
        for r in range(2):
            part = wide[:, r * LANES : (r + 1) * LANES]
            spot = pl.ds((2 * d + r) * rows, rows)
            for c in range(blocks):
                block = part[c * rows : (c + 1) * rows]
                if c == 0:
                    block = jnp.where(left, part[blocks * rows :], block)
                hi_w, lo_w = split(block)
                w_hi[spot, c * LANES : (c + 1) * LANES] = hi_w
                w_lo[spot, c * LANES : (c + 1) * LANES] = lo_w
    image = dot(row_hi, w_hi[...]) + dot(row_lo, w_hi[...]) + dot(row_hi, w_lo[...])
    return image[:rows] - target, image[rows:]


def adjoint(residual, adj_rows, adj, volume, emit):
    planes = len(volume)
    rows, width = volume[0].shape
    blocks = width // LANES
    hi, lo = split(residual)
    upper = dot(adj_rows, jnp.concatenate([hi, lo, hi], axis=0))
    left = lane_iota((rows, LANES)) < HALF
    result = []
    for d in range(planes):
        total = None
        for r in range(2):
            spot = (2 * d + r) * rows
            part = upper[spot : spot + rows]
            edge = part[:, :LANES]
            column = [jnp.where(left, 0.0, edge)]
            column += [part[:, b * LANES : (b + 1) * LANES] for b in range(1, blocks)]
            column += [jnp.where(left, edge, 0.0)]
            for side in split(jnp.concatenate(column, axis=0)):
                side = jnp.concatenate([side[:-rows], side[rows:]], axis=1)
                term = dot(side, adj[d, r])
                total = term if total is None else total + term
        grad = total[:, :LANES] + total[:, LANES:]
        grad = jnp.concatenate([grad[c * rows : (c + 1) * rows] for c in range(blocks)], axis=1)
        moved = volume[d] - descent_step * grad
        plane = moved - jnp.clip(moved, -shrinkage, shrinkage)
        emit(d, plane)
        result.append(plane)
    return result


def window_target(measured, place):
    reach = measured.shape[0] // 2
    upper = jnp.where(place.flag == 1, measured[reach:], 0.0)
    lower = jnp.where(place.flag == 1, 0.0, measured[:reach])
    return pltpu.roll(jnp.concatenate([upper, lower], axis=0), HALF, 1)


def joined(place, kept, crossed, swapped):
    add = jnp.where(place.end_even, swapped, jnp.where(place.end_odd, 0.0, crossed))
    other = jnp.where(
        place.end_even, crossed, jnp.where(place.end_odd, crossed + swapped, swapped)
    )
    return kept + add, other


def first_kernel(
    paired, view, index, row_bank, col_bank, volume, measured, mine, other, taps,
    index_v, row_v, col_v, volume_v, measured_v, fwd_hi, fwd_lo, w_hi, w_lo, sems,
):
    pairs = [
        (index, index_v), (col_bank, col_v), (row_bank, row_v), (volume, volume_v),
        (measured.at[0], measured_v),
    ]
    copies = [pltpu.make_async_copy(a, b, sems.at[i]) for i, (a, b) in enumerate(pairs)]
    for copy in copies:
        copy.start()
    place = Place(paired)
    planes = volume.shape[0]
    reach = (row_bank.shape[0] - 1) // 2
    for copy in copies[:3]:
        copy.wait()
    pick_taps(view.shape[0], planes, view, index_v[...], (row_v, col_v), taps)
    for d in range(planes):
        column_operands(taps, d, d, reach, (fwd_hi, fwd_lo), None)
    row_hi, row_lo = split(row_operand(taps, 0, planes, reach, place))
    for copy in copies[3:]:
        copy.wait()
    target = window_target(measured_v[...], place) if paired else 0.0
    mine[...], other[...] = forward(
        [volume_v[d] for d in range(planes)], fwd_hi, fwd_lo, row_hi, row_lo, target, w_hi, w_lo
    )


def prepare_kernel(paired, planes, reach, back, ahead, taps, *outs):
    place = Place(paired)
    fwd_hi, fwd_lo, row_hi, row_lo = outs[:4]
    wanted = sorted(set(back) | {ahead})
    for step in wanted:
        adj, adj_rows = outs[4 + 2 * back.index(step) :][:2] if step in back else (None, None)
        for d in range(planes):
            column_operands(
                taps, step * planes + d, d, reach, (fwd_hi, fwd_lo) if step == ahead else None, adj
            )
        stack = row_operand(taps, step, planes, reach, place)
        if step == ahead:
            row_hi[...], row_lo[...] = split(stack)
        if step in back:
            adj_rows[...] = adjoint_row_operand(stack)


def middle_kernel(
    paired, step, kept, crossed, swapped, adj, adj_rows, fwd_hi, fwd_lo, row_hi, row_lo,
    volume, measured, mine, other, fresh, w_hi, w_lo,
):
    place = Place(paired)
    residual = jnp.concatenate(joined(place, kept[...], crossed[...], swapped[...]), axis=0)

    def emit(d, plane):
        fresh[d] = plane

    planes = [volume[d] for d in range(volume.shape[0])]
    planes = adjoint(residual, adj_rows[...], adj, planes, emit)
    target = window_target(measured[step], place) if paired else 0.0
    mine[...], other[...] = forward(
        planes, fwd_hi, fwd_lo, row_hi[...], row_lo[...], target, w_hi, w_lo
    )


def last_kernel(
    paired, kept, crossed, swapped, adj, adj_rows, volume, fresh, residual_out,
    fresh_v, residual_v, sems,
):
    place = Place(paired)
    mine, other = joined(place, kept[...], crossed[...], swapped[...])
    reach = mine.shape[0] // 2
    lower = place.flag == 1
    own = jnp.concatenate(
        [jnp.where(lower, other[reach:], mine[reach:]), jnp.where(lower, mine[:reach], other[:reach])],
        axis=0,
    )
    residual_v[...] = pltpu.roll(own, own.shape[1] - HALF, 1)
    count = volume.shape[0]
    copies = [pltpu.make_async_copy(fresh_v.at[d], fresh.at[d], sems.at[d]) for d in range(count)]
    copies.append(pltpu.make_async_copy(residual_v, residual_out, sems.at[count]))
    copies[count].start()

    def emit(d, plane):
        fresh_v[d] = plane
        copies[d].start()

    planes = [volume[d] for d in range(count)]
    adjoint(jnp.concatenate([mine, other], axis=0), adj_rows[...], adj, planes, emit)
    for copy in copies:
        copy.wait()


VMEM = pl.BlockSpec(memory_space=pltpu.VMEM)
SMEM = pl.BlockSpec(memory_space=pltpu.SMEM)
HBM = pl.BlockSpec(memory_space=pltpu.HBM)


def call(kernel, in_specs, out_specs, outs, scratch, flops, name, args):
    return pl.pallas_call(
        kernel,
        out_shape=outs,
        in_specs=in_specs,
        out_specs=out_specs,
        scratch_shapes=scratch,
        compiler_params=pltpu.CompilerParams(vmem_limit_bytes=24 << 20),
        cost_estimate=pl.CostEstimate(flops=flops, bytes_accessed=4 << 20, transcendentals=0),
        name=name,
    )(*args)


def per_device(volume, measured, row_bank, col_bank, kernel_index, view_order):
    planes, rows, width = volume.shape
    steps = measured.shape[0]
    reach = (row_bank.shape[2] - 1) // 2
    assert rows == 2 * reach and width % LANES == 0 and reach <= HALF
    depth, tiles = lax.axis_size("depth"), lax.axis_size("tile")
    d, t = lax.axis_index("depth"), lax.axis_index("tile")
    paired = depth == 2 and tiles % 2 == 0 and tiles > 2
    place = Place(paired)

    def flow(spot):
        side, i = divmod(spot, tiles)
        ends = (0, tiles - 1)
        if side == 1:
            return i if i in ends else tiles + (i + 1 if i % 2 else i - 1)
        return tiles + (i ^ 1) if (i ^ 1) in ends else i ^ 1

    def exchange(mine, other, step, during):
        if paired:
            swap = [(0, 1), (1, 0)]
            kept = mine + lax.ppermute(other, "depth", swap)
            crossed = lax.ppermute(
                kept, ("depth", "tile"), [(i, flow(i)) for i in range(2 * tiles)]
            )
            ready = during()
            if ready:
                crossed, *ready = lax.optimization_barrier((crossed, *ready))
            send = jnp.where(place.end_odd, 0.0, kept) + jnp.where(place.end_even, 0.0, crossed)
            return kept, crossed, lax.ppermute(send, "depth", swap), ready
        target = jnp.roll(measured[step], HALF, axis=1)
        high = jnp.pad(target[:reach], ((reach, 0), (0, 0)))
        low = jnp.pad(target[reach:], ((0, reach), (0, 0)))
        lower = place.flag == 1
        evens = [(i, i ^ 1) for i in range(tiles) if i ^ 1 < tiles]
        odds = [(i, i + 1 if i % 2 else i - 1) for i in range(tiles)]
        odds = [(i, j) for i, j in odds if 0 <= j < tiles]
        kept = lax.psum(mine, "depth") - jnp.where(lower, low, high)
        rest = lax.psum(other, "depth") - jnp.where(lower, high, low)
        rest = rest + lax.ppermute(rest, "tile", odds)
        return kept, lax.ppermute(kept, "tile", evens), rest, during()

    shape = jax.ShapeDtypeStruct
    stacks = 2 * planes * rows
    forward_shapes = [
        shape((planes, 2 * LANES, 2 * LANES), bf16),
        shape((planes, 2 * LANES, 2 * LANES), bf16),
        shape((2 * rows, stacks), bf16),
        shape((2 * rows, stacks), bf16),
    ]
    adjoint_shapes = [
        shape((planes, 2, 2 * LANES, 2 * LANES), bf16),
        shape((stacks, 6 * rows), bf16),
    ]
    image = shape((rows, width), f32)
    block = shape(volume.shape, f32)
    lines = -(-steps * planes // 16) * 16
    tap_shape = shape((4, lines, LANES), f32)
    scratch = [pltpu.VMEM((stacks, width), bf16)] * 2
    work = 400 << 20

    index = kernel_index.T
    banks = [jnp.transpose(x, (2, 1, 0)) for x in (row_bank, col_bank)]
    mine, other, taps = call(
        functools.partial(first_kernel, paired), [SMEM] + [HBM] * 5, [VMEM] * 3,
        [image, image, tap_shape],
        [pltpu.VMEM(x.shape, x.dtype) for x in (index, *banks, volume, measured[0])]
        + [pltpu.VMEM(x.shape, x.dtype) for x in forward_shapes[:2]]
        + scratch + [pltpu.SemaphoreType.DMA((5,))],
        work, "first", (view_order, index, *banks, volume, measured),
    )

    def prepare(back, ahead):
        outs = forward_shapes + adjoint_shapes * len(back)
        return call(
            functools.partial(prepare_kernel, paired, planes, reach, back, ahead),
            [VMEM], [VMEM] * len(outs), outs, [], work, "prepare", (taps,),
        )

    adjoints = []
    for step in range(1, steps):
        back = (0, 1) if step == 1 else (step,)
        kept, crossed, swapped, ready = exchange(
            mine, other, step - 1, lambda: prepare(back, step)
        )
        forwards = ready[:4]
        adjoints += [ready[i : i + 2] for i in range(4, len(ready), 2)]
        mine, other, volume = call(
            functools.partial(middle_kernel, paired, step), [VMEM] * 11, [VMEM] * 3,
            [image, image, block], scratch, 2 * work, "middle",
            (kept, crossed, swapped, *adjoints[step - 1], *forwards, volume, measured),
        )
    kept, crossed, swapped, _ = exchange(mine, other, steps - 1, lambda: [])
    return call(
        functools.partial(last_kernel, paired), [VMEM] * 6, [HBM] * 2, [block, image],
        [pltpu.VMEM(volume.shape, f32), pltpu.VMEM((rows, width), f32),
         pltpu.SemaphoreType.DMA((planes + 1,))],
        work, "last", (kept, crossed, swapped, *adjoints[steps - 1], volume),
    )


def solution(mesh):
    return jax.shard_map(
        per_device,
        mesh=mesh,
        in_specs=(P("depth", "tile", None), P(None, "tile", None), P(), P(), P(None, "depth"), P()),
        out_specs=(P("depth", "tile", None), P("tile", None)),
        check_vma=False,
    )
```

```python
import functools

import jax
import jax.numpy as jnp
from jax import lax
from jax.experimental import pallas as pl
from jax.experimental.pallas import tpu as pltpu
from jax.sharding import PartitionSpec as P

descent_step = 0.5
shrinkage = 0.1
LANES = 128
HALF = LANES // 2
bf16, f32 = jnp.bfloat16, jnp.float32


def split(x):
    hi = x.astype(bf16)
    return hi, (x - hi.astype(f32)).astype(bf16)


def dot(a, b):
    return lax.dot_general(a, b, (((1,), (0,)), ((), ())), preferred_element_type=f32)


def dot_nt(a, b):
    return lax.dot_general(a, b, (((1,), (1,)), ((), ())), preferred_element_type=f32)


def lane_iota(shape):
    return lax.broadcasted_iota(jnp.int32, shape, 1)


def row_iota(shape):
    return lax.broadcasted_iota(jnp.int32, shape, 0)


class Place:
    def __init__(self, paired):
        d, t = lax.axis_index("depth"), lax.axis_index("tile")
        tiles = lax.axis_size("tile")
        odd = lax.rem(t, 2)
        self.first = t == 0
        self.last = t == tiles - 1
        self.flag = 1 - jnp.bitwise_xor(odd, d) if paired else 1 - odd
        end = jnp.logical_and(jnp.logical_or(self.first, self.last), paired)
        self.end_even = jnp.logical_and(end, d == 0)
        self.end_odd = jnp.logical_and(end, d == 1)


def pick_taps(steps, planes, view_ref, index, banks, taps_ref):
    count = taps_ref.shape[1]
    index = index.astype(f32)
    copies = jnp.concatenate([index] * (count // planes), axis=0)
    line, lane = row_iota(copies.shape), lane_iota(copies.shape)
    view = jnp.full(copies.shape, view_ref[0], jnp.int32)
    for step in range(1, steps):
        view = jnp.where(line >= step * planes, view_ref[step], view)
    entry = jnp.sum(jnp.where(lane == view, copies, 0.0), axis=1, keepdims=True)
    size = banks[0].shape[2]
    chosen = (lane_iota((count, size)).astype(f32) == entry).astype(f32).astype(bf16)
    taps_ref[...] = jnp.zeros(taps_ref.shape, f32)
    for b, bank in enumerate(banks):
        for r in range(2):
            hi, lo = split(bank[:, r, :])
            taps = dot_nt(chosen, hi) + dot_nt(chosen, lo)
            taps_ref[2 * b + r, :, 0 : taps.shape[1]] = taps


def column_operands(taps_ref, line, d, reach, forward_out, adjoint_out):
    square = (LANES, LANES)
    below = lane_iota(square) < row_iota(square)
    above = lane_iota(square) > row_iota(square)
    for r in range(2):
        base = pltpu.roll(
            jnp.broadcast_to(taps_ref[2 + r, line : line + 1], (8, LANES)),
            (LANES - HALF - reach) % LANES, 1, stride=1, stride_axis=0,
        )
        ring = jnp.concatenate(
            [base] + [pltpu.roll(base, 8 * b, 1) for b in range(1, LANES // 8)], axis=0
        )
        low_hi, low_lo = split(jnp.where(below, ring, 0.0))
        up_hi, up_lo = split(jnp.where(above, ring, 0.0))
        left, right = slice(0, LANES), slice(LANES, 2 * LANES)
        if forward_out is not None:
            fwd_hi, fwd_lo = forward_out
            here = slice(r * LANES, (r + 1) * LANES)
            fwd_hi[d, here, left] = up_hi
            fwd_hi[d, here, right] = low_hi
            fwd_lo[d, here, left] = up_lo
            fwd_lo[d, here, right] = low_lo
        if adjoint_out is not None:
            adjoint_out[d, r, left, left] = low_hi
            adjoint_out[d, r, left, right] = low_lo
            adjoint_out[d, r, right, left] = up_hi
            adjoint_out[d, r, right, right] = up_lo


def row_operand(taps_ref, step, planes, reach, place):
    rows = 2 * reach
    per_lane = LANES // rows
    window, lane = row_iota((8, LANES)), lane_iota((8, LANES)) // rows
    parts = []
    for k in range(2 * planes):
        line = step * planes + k // 2
        parts.append(
            pltpu.roll(
                jnp.broadcast_to(taps_ref[k % 2, line : line + 1], (8, LANES)),
                ((k % per_lane) * rows - 2 * reach) % LANES, 1, stride=1, stride_axis=0,
            )
        )
    bands = []
    for band in range(2 * rows // 8):
        start = (8 * band) % rows
        offset = start + rows * (place.flag if band < rows // 8 else 1 - place.flag)
        spot = window + offset
        good = jnp.logical_and(
            jnp.logical_or(jnp.logical_not(place.first), spot >= reach),
            jnp.logical_or(jnp.logical_not(place.last), spot < rows + reach),
        )
        line = []
        for group in range(2 * planes // per_lane):
            total = jnp.zeros((8, LANES), f32)
            for k in range(per_lane):
                part = pltpu.roll(parts[group * per_lane + k], offset, 1)
                total = jnp.where(lane == k, part, total)
            line.append(jnp.where(good, total, 0.0))
        bands.append(jnp.concatenate(line, axis=1))
    return jnp.concatenate(bands, axis=0)


def adjoint_row_operand(stack):
    hi, lo = split(stack.T)
    return jnp.concatenate([hi, hi, lo], axis=1)


def forward(volume, fwd_hi, fwd_lo, row_hi, row_lo, target, w_hi, w_lo):
    planes = len(volume)
    rows, width = volume[0].shape
    blocks = width // LANES
    zero = jnp.zeros((rows, LANES), bf16)
    left = lane_iota((rows, LANES)) < HALF
    for d in range(planes):
        sides = []
        for part in split(volume[d]):
            column = [zero] + [part[:, b * LANES : (b + 1) * LANES] for b in range(blocks)] + [zero]
            column = jnp.concatenate(column, axis=0)
            sides.append(jnp.concatenate([column[:-rows], column[rows:]], axis=1))
        hi, lo = sides
        wide = dot_nt(hi, fwd_hi[d]) + dot_nt(lo, fwd_hi[d]) + dot_nt(hi, fwd_lo[d])
        for r in range(2):
            part = wide[:, r * LANES : (r + 1) * LANES]
            spot = pl.ds((2 * d + r) * rows, rows)
            for c in range(blocks):
                block = part[c * rows : (c + 1) * rows]
                if c == 0:
                    block = jnp.where(left, part[blocks * rows :], block)
                hi_w, lo_w = split(block)
                w_hi[spot, c * LANES : (c + 1) * LANES] = hi_w
                w_lo[spot, c * LANES : (c + 1) * LANES] = lo_w
    image = dot(row_hi, w_hi[...]) + dot(row_lo, w_hi[...]) + dot(row_hi, w_lo[...])
    return image[:rows] - target, image[rows:]


def adjoint(residual, adj_rows, adj, volume, emit):
    planes = len(volume)
    rows, width = volume[0].shape
    blocks = width // LANES
    hi, lo = split(residual)
    upper = dot(adj_rows, jnp.concatenate([hi, lo, hi], axis=0))
    left = lane_iota((rows, LANES)) < HALF
    result = []
    for d in range(planes):
        total = None
        for r in range(2):
            spot = (2 * d + r) * rows
            part = upper[spot : spot + rows]
            edge = part[:, :LANES]
            column = [jnp.where(left, 0.0, edge)]
            column += [part[:, b * LANES : (b + 1) * LANES] for b in range(1, blocks)]
            column += [jnp.where(left, edge, 0.0)]
            for side in split(jnp.concatenate(column, axis=0)):
                side = jnp.concatenate([side[:-rows], side[rows:]], axis=1)
                term = dot(side, adj[d, r])
                total = term if total is None else total + term
        grad = total[:, :LANES] + total[:, LANES:]
        grad = jnp.concatenate([grad[c * rows : (c + 1) * rows] for c in range(blocks)], axis=1)
        moved = volume[d] - descent_step * grad
        plane = moved - jnp.clip(moved, -shrinkage, shrinkage)
        emit(d, plane)
        result.append(plane)
    return result


def window_target(measured, place):
    reach = measured.shape[0] // 2
    upper = jnp.where(place.flag == 1, measured[reach:], 0.0)
    lower = jnp.where(place.flag == 1, 0.0, measured[:reach])
    return pltpu.roll(jnp.concatenate([upper, lower], axis=0), HALF, 1)


def joined(place, kept, crossed, swapped):
    add = jnp.where(place.end_even, swapped, jnp.where(place.end_odd, 0.0, crossed))
    other = jnp.where(
        place.end_even, crossed, jnp.where(place.end_odd, crossed + swapped, swapped)
    )
    return kept + add, other


def first_kernel(
    paired, view_h, index, row_bank, col_bank, volume, measured, mine, other, taps,
    view, index_v, row_v, col_v, volume_v, measured_v, fwd_hi, fwd_lo, w_hi, w_lo, sems,
):
    pairs = [
        (view_h, view), (index, index_v), (col_bank, col_v), (row_bank, row_v),
        (volume, volume_v), (measured.at[0], measured_v),
    ]
    copies = [pltpu.make_async_copy(a, b, sems.at[i]) for i, (a, b) in enumerate(pairs)]
    for copy in copies:
        copy.start()
    place = Place(paired)
    planes = volume.shape[0]
    reach = (row_bank.shape[0] - 1) // 2
    for copy in copies[:4]:
        copy.wait()
    pick_taps(view.shape[0], planes, view, index_v[...], (row_v, col_v), taps)
    for d in range(planes):
        column_operands(taps, d, d, reach, (fwd_hi, fwd_lo), None)
    row_hi, row_lo = split(row_operand(taps, 0, planes, reach, place))
    for copy in copies[4:]:
        copy.wait()
    target = window_target(measured_v[...], place) if paired else 0.0
    mine[...], other[...] = forward(
        [volume_v[d] for d in range(planes)], fwd_hi, fwd_lo, row_hi, row_lo, target, w_hi, w_lo
    )


def prepare_kernel(paired, planes, reach, back, ahead, taps, *outs):
    place = Place(paired)
    fwd_hi, fwd_lo, row_hi, row_lo = outs[:4]
    wanted = sorted(set(back) | {ahead})
    for step in wanted:
        adj, adj_rows = outs[4 + 2 * back.index(step) :][:2] if step in back else (None, None)
        for d in range(planes):
            column_operands(
                taps, step * planes + d, d, reach, (fwd_hi, fwd_lo) if step == ahead else None, adj
            )
        stack = row_operand(taps, step, planes, reach, place)
        if step == ahead:
            row_hi[...], row_lo[...] = split(stack)
        if step in back:
            adj_rows[...] = adjoint_row_operand(stack)


def middle_kernel(
    paired, step, kept, crossed, swapped, adj, adj_rows, fwd_hi, fwd_lo, row_hi, row_lo,
    volume, measured, mine, other, fresh, w_hi, w_lo,
):
    place = Place(paired)
    residual = jnp.concatenate(joined(place, kept[...], crossed[...], swapped[...]), axis=0)

    def emit(d, plane):
        fresh[d] = plane

    planes = [volume[d] for d in range(volume.shape[0])]
    planes = adjoint(residual, adj_rows[...], adj, planes, emit)
    target = window_target(measured[step], place) if paired else 0.0
    mine[...], other[...] = forward(
        planes, fwd_hi, fwd_lo, row_hi[...], row_lo[...], target, w_hi, w_lo
    )


def last_kernel(
    paired, kept, crossed, swapped, adj, adj_rows, volume, fresh, residual_out,
    fresh_v, residual_v, sems,
):
    place = Place(paired)
    mine, other = joined(place, kept[...], crossed[...], swapped[...])
    reach = mine.shape[0] // 2
    lower = place.flag == 1
    own = jnp.concatenate(
        [jnp.where(lower, other[reach:], mine[reach:]), jnp.where(lower, mine[:reach], other[:reach])],
        axis=0,
    )
    residual_v[...] = pltpu.roll(own, own.shape[1] - HALF, 1)
    count = volume.shape[0]
    copies = [pltpu.make_async_copy(fresh_v.at[d], fresh.at[d], sems.at[d]) for d in range(count)]
    copies.append(pltpu.make_async_copy(residual_v, residual_out, sems.at[count]))
    copies[count].start()

    def emit(d, plane):
        fresh_v[d] = plane
        copies[d].start()

    planes = [volume[d] for d in range(count)]
    adjoint(jnp.concatenate([mine, other], axis=0), adj_rows[...], adj, planes, emit)
    for copy in copies:
        copy.wait()


VMEM = pl.BlockSpec(memory_space=pltpu.VMEM)
HBM = pl.BlockSpec(memory_space=pltpu.HBM)


def call(kernel, in_specs, out_specs, outs, scratch, flops, name, args):
    return pl.pallas_call(
        kernel,
        out_shape=outs,
        in_specs=in_specs,
        out_specs=out_specs,
        scratch_shapes=scratch,
        compiler_params=pltpu.CompilerParams(vmem_limit_bytes=24 << 20),
        cost_estimate=pl.CostEstimate(flops=flops, bytes_accessed=4 << 20, transcendentals=0),
        name=name,
    )(*args)


def per_device(volume, measured, row_bank, col_bank, kernel_index, view_order):
    planes, rows, width = volume.shape
    steps = measured.shape[0]
    reach = (row_bank.shape[2] - 1) // 2
    assert rows == 2 * reach and width % LANES == 0 and reach <= HALF
    depth, tiles = lax.axis_size("depth"), lax.axis_size("tile")
    d, t = lax.axis_index("depth"), lax.axis_index("tile")
    paired = depth == 2 and tiles % 2 == 0 and tiles > 2
    place = Place(paired)

    def flow(spot):
        side, i = divmod(spot, tiles)
        ends = (0, tiles - 1)
        if side == 1:
            return i if i in ends else tiles + (i + 1 if i % 2 else i - 1)
        return tiles + (i ^ 1) if (i ^ 1) in ends else i ^ 1

    def exchange(mine, other, step, during):
        if paired:
            swap = [(0, 1), (1, 0)]
            kept = mine + lax.ppermute(other, "depth", swap)
            crossed = lax.ppermute(
                kept, ("depth", "tile"), [(i, flow(i)) for i in range(2 * tiles)]
            )
            ready = during()
            if ready:
                crossed, *ready = lax.optimization_barrier((crossed, *ready))
            send = jnp.where(place.end_odd, 0.0, kept) + jnp.where(place.end_even, 0.0, crossed)
            return kept, crossed, lax.ppermute(send, "depth", swap), ready
        target = jnp.roll(measured[step], HALF, axis=1)
        high = jnp.pad(target[:reach], ((reach, 0), (0, 0)))
        low = jnp.pad(target[reach:], ((0, reach), (0, 0)))
        lower = place.flag == 1
        evens = [(i, i ^ 1) for i in range(tiles) if i ^ 1 < tiles]
        odds = [(i, i + 1 if i % 2 else i - 1) for i in range(tiles)]
        odds = [(i, j) for i, j in odds if 0 <= j < tiles]
        kept = lax.psum(mine, "depth") - jnp.where(lower, low, high)
        rest = lax.psum(other, "depth") - jnp.where(lower, high, low)
        rest = rest + lax.ppermute(rest, "tile", odds)
        return kept, lax.ppermute(kept, "tile", evens), rest, during()

    shape = jax.ShapeDtypeStruct
    stacks = 2 * planes * rows
    forward_shapes = [
        shape((planes, 2 * LANES, 2 * LANES), bf16),
        shape((planes, 2 * LANES, 2 * LANES), bf16),
        shape((2 * rows, stacks), bf16),
        shape((2 * rows, stacks), bf16),
    ]
    adjoint_shapes = [
        shape((planes, 2, 2 * LANES, 2 * LANES), bf16),
        shape((stacks, 6 * rows), bf16),
    ]
    image = shape((rows, width), f32)
    block = shape(volume.shape, f32)
    lines = -(-steps * planes // 16) * 16
    tap_shape = shape((4, lines, LANES), f32)
    scratch = [pltpu.VMEM((stacks, width), bf16)] * 2
    work = 400 << 20

    index = kernel_index.T
    banks = [jnp.transpose(x, (2, 1, 0)) for x in (row_bank, col_bank)]
    mine, other, taps = call(
        functools.partial(first_kernel, paired), [HBM] * 6, [VMEM] * 3,
        [image, image, tap_shape],
        [pltpu.SMEM(view_order.shape, jnp.int32)]
        + [pltpu.VMEM(x.shape, x.dtype) for x in (index, *banks, volume, measured[0])]
        + [pltpu.VMEM(x.shape, x.dtype) for x in forward_shapes[:2]]
        + scratch + [pltpu.SemaphoreType.DMA((6,))],
        work, "first",
        [pltpu.with_memory_space_constraint(x, pltpu.HBM)
         for x in (view_order, index, *banks, volume, measured)],
    )

    def prepare(back, ahead):
        outs = forward_shapes + adjoint_shapes * len(back)
        return call(
            functools.partial(prepare_kernel, paired, planes, reach, back, ahead),
            [VMEM], [VMEM] * len(outs), outs, [], work, "prepare", (taps,),
        )

    adjoints = []
    for step in range(1, steps):
        back = (0, 1) if step == 1 else (step,)
        kept, crossed, swapped, ready = exchange(
            mine, other, step - 1, lambda: prepare(back, step)
        )
        forwards = ready[:4]
        adjoints += [ready[i : i + 2] for i in range(4, len(ready), 2)]
        mine, other, volume = call(
            functools.partial(middle_kernel, paired, step), [VMEM] * 11, [VMEM] * 3,
            [image, image, block], scratch, 2 * work, "middle",
            (kept, crossed, swapped, *adjoints[step - 1], *forwards, volume, measured),
        )
    kept, crossed, swapped, _ = exchange(mine, other, steps - 1, lambda: [])
    return call(
        functools.partial(last_kernel, paired), [VMEM] * 6, [HBM] * 2, [block, image],
        [pltpu.VMEM(volume.shape, f32), pltpu.VMEM((rows, width), f32),
         pltpu.SemaphoreType.DMA((planes + 1,))],
        work, "last", (kept, crossed, swapped, *adjoints[steps - 1], volume),
    )


def solution(mesh):
    return jax.shard_map(
        per_device,
        mesh=mesh,
        in_specs=(P("depth", "tile", None), P(None, "tile", None), P(), P(), P(None, "depth"), P()),
        out_specs=(P("depth", "tile", None), P("tile", None)),
        check_vma=False,
    )
```

```python
import functools

import jax
import jax.numpy as jnp
from jax import lax
from jax.experimental import pallas as pl
from jax.experimental.pallas import tpu as pltpu
from jax.sharding import PartitionSpec as P

descent_step = 0.5
shrinkage = 0.1
LANES = 128
HALF = LANES // 2
bf16, f32 = jnp.bfloat16, jnp.float32


def split(x):
    hi = x.astype(bf16)
    return hi, (x - hi.astype(f32)).astype(bf16)


def dot(a, b):
    return lax.dot_general(a, b, (((1,), (0,)), ((), ())), preferred_element_type=f32)


def dot_nt(a, b):
    return lax.dot_general(a, b, (((1,), (1,)), ((), ())), preferred_element_type=f32)


def lane_iota(shape):
    return lax.broadcasted_iota(jnp.int32, shape, 1)


def row_iota(shape):
    return lax.broadcasted_iota(jnp.int32, shape, 0)


class Place:
    def __init__(self, paired):
        d, t = lax.axis_index("depth"), lax.axis_index("tile")
        tiles = lax.axis_size("tile")
        odd = lax.rem(t, 2)
        self.first = t == 0
        self.last = t == tiles - 1
        end = jnp.logical_or(self.first, self.last)
        side = jnp.where(end, 1 - d, d)
        self.flag = 1 - jnp.bitwise_xor(odd, side) if paired else 1 - odd
        end = jnp.logical_and(end, paired)
        self.end_even = jnp.logical_and(end, side == 0)
        self.end_odd = jnp.logical_and(end, side == 1)


def pick_taps(steps, planes, view_ref, index, banks, taps_ref):
    count = taps_ref.shape[1]
    index = index.astype(f32)
    copies = jnp.concatenate([index] * (count // planes), axis=0)
    line, lane = row_iota(copies.shape), lane_iota(copies.shape)
    view = jnp.full(copies.shape, view_ref[0], jnp.int32)
    for step in range(1, steps):
        view = jnp.where(line >= step * planes, view_ref[step], view)
    entry = jnp.sum(jnp.where(lane == view, copies, 0.0), axis=1, keepdims=True)
    size = banks[0].shape[2]
    chosen = (lane_iota((count, size)).astype(f32) == entry).astype(f32).astype(bf16)
    taps_ref[...] = jnp.zeros(taps_ref.shape, f32)
    for b, bank in enumerate(banks):
        for r in range(2):
            hi, lo = split(bank[r])
            taps = dot_nt(chosen, hi) + dot_nt(chosen, lo)
            taps_ref[2 * b + r, :, 0 : taps.shape[1]] = taps


def column_operands(taps_ref, line, d, reach, forward_out, adjoint_out):
    square = (LANES, LANES)
    below = (lane_iota(square) < row_iota(square)).astype(f32).astype(bf16)
    above = (lane_iota(square) > row_iota(square)).astype(f32).astype(bf16)
    for r in range(2):
        base = pltpu.roll(
            jnp.broadcast_to(taps_ref[2 + r, line : line + 1], (8, LANES)),
            (LANES - HALF - reach) % LANES, 1, stride=1, stride_axis=0,
        )
        ring = jnp.concatenate(
            [base] + [pltpu.roll(base, 8 * b, 1) for b in range(1, LANES // 8)], axis=0
        )
        hi, lo = split(ring)
        low_hi, low_lo, up_hi, up_lo = hi * below, lo * below, hi * above, lo * above
        left, right = slice(0, LANES), slice(LANES, 2 * LANES)
        if forward_out is not None:
            fwd_hi, fwd_lo = forward_out
            here = slice(r * LANES, (r + 1) * LANES)
            fwd_hi[d, here, left] = up_hi
            fwd_hi[d, here, right] = low_hi
            fwd_lo[d, here, left] = up_lo
            fwd_lo[d, here, right] = low_lo
        if adjoint_out is not None:
            adjoint_out[d, r, left, left] = low_hi
            adjoint_out[d, r, left, right] = low_lo
            adjoint_out[d, r, right, left] = up_hi
            adjoint_out[d, r, right, right] = up_lo


def row_operand(taps_ref, step, planes, reach, place):
    rows = 2 * reach
    per_lane = LANES // rows
    window, lane = row_iota((8, LANES)), lane_iota((8, LANES)) // rows
    parts = []
    for k in range(2 * planes):
        line = step * planes + k // 2
        parts.append(
            pltpu.roll(
                jnp.broadcast_to(taps_ref[k % 2, line : line + 1], (8, LANES)),
                ((k % per_lane) * rows - 2 * reach) % LANES, 1, stride=1, stride_axis=0,
            )
        )
    bands = []
    for band in range(2 * rows // 8):
        start = (8 * band) % rows
        offset = start + rows * (place.flag if band < rows // 8 else 1 - place.flag)
        spot = window + offset
        good = jnp.logical_and(
            jnp.logical_or(jnp.logical_not(place.first), spot >= reach),
            jnp.logical_or(jnp.logical_not(place.last), spot < rows + reach),
        )
        line = []
        for group in range(2 * planes // per_lane):
            total = jnp.zeros((8, LANES), f32)
            for k in range(per_lane):
                part = pltpu.roll(parts[group * per_lane + k], offset, 1)
                total = jnp.where(lane == k, part, total)
            line.append(jnp.where(good, total, 0.0))
        bands.append(jnp.concatenate(line, axis=1))
    return jnp.concatenate(bands, axis=0)


def adjoint_row_operand(stack):
    hi, lo = split(stack.T)
    return jnp.concatenate([hi, hi, lo], axis=1)


def forward(volume, fwd_hi, fwd_lo, row_hi, row_lo, target, w_hi, w_lo):
    planes = len(volume)
    rows, width = volume[0].shape
    blocks = width // LANES
    zero = jnp.zeros((rows, LANES), bf16)
    left = lane_iota((rows, LANES)) < HALF
    for d in range(planes):
        sides = []
        for part in split(volume[d]):
            column = [zero] + [part[:, b * LANES : (b + 1) * LANES] for b in range(blocks)] + [zero]
            column = jnp.concatenate(column, axis=0)
            sides.append(jnp.concatenate([column[:-rows], column[rows:]], axis=1))
        hi, lo = sides
        wide = dot_nt(hi, fwd_hi[d]) + dot_nt(lo, fwd_hi[d]) + dot_nt(hi, fwd_lo[d])
        for r in range(2):
            part = wide[:, r * LANES : (r + 1) * LANES]
            spot = pl.ds((2 * d + r) * rows, rows)
            for c in range(blocks):
                block = part[c * rows : (c + 1) * rows]
                if c == 0:
                    block = jnp.where(left, part[blocks * rows :], block)
                hi_w, lo_w = split(block)
                w_hi[spot, c * LANES : (c + 1) * LANES] = hi_w
                w_lo[spot, c * LANES : (c + 1) * LANES] = lo_w
    image = dot(row_hi, w_hi[...]) + dot(row_lo, w_hi[...]) + dot(row_hi, w_lo[...])
    return image[:rows] - target, image[rows:]


def adjoint(residual, adj_rows, adj, volume, emit):
    planes = len(volume)
    rows, width = volume[0].shape
    blocks = width // LANES
    hi, lo = split(residual)
    upper = dot(adj_rows, jnp.concatenate([hi, lo, hi], axis=0))
    left = lane_iota((rows, LANES)) < HALF
    result = []
    for d in range(planes):
        total = None
        for r in range(2):
            spot = (2 * d + r) * rows
            part = upper[spot : spot + rows]
            edge = part[:, :LANES]
            column = [jnp.where(left, 0.0, edge)]
            column += [part[:, b * LANES : (b + 1) * LANES] for b in range(1, blocks)]
            column += [jnp.where(left, edge, 0.0)]
            for side in split(jnp.concatenate(column, axis=0)):
                side = jnp.concatenate([side[:-rows], side[rows:]], axis=1)
                term = dot(side, adj[d, r])
                total = term if total is None else total + term
        grad = total[:, :LANES] + total[:, LANES:]
        grad = jnp.concatenate([grad[c * rows : (c + 1) * rows] for c in range(blocks)], axis=1)
        moved = volume[d] - descent_step * grad
        plane = moved - jnp.clip(moved, -shrinkage, shrinkage)
        emit(d, plane)
        result.append(plane)
    return result


def window_target(measured, place):
    reach = measured.shape[0] // 2
    upper = jnp.where(place.flag == 1, measured[reach:], 0.0)
    lower = jnp.where(place.flag == 1, 0.0, measured[:reach])
    return pltpu.roll(jnp.concatenate([upper, lower], axis=0), HALF, 1)


def joined(place, kept, crossed, swapped):
    add = jnp.where(place.end_even, swapped, jnp.where(place.end_odd, 0.0, crossed))
    other = jnp.where(
        place.end_even, crossed, jnp.where(place.end_odd, crossed + swapped, swapped)
    )
    return kept + add, other


def first_kernel(
    paired, view_h, index, row_bank, col_bank, volume, measured, mine, other, taps,
    view, index_v, row_v, col_v, volume_v, measured_v, fwd_hi, fwd_lo, w_hi, w_lo, sems,
):
    pairs = [(view_h, view), (index, index_v)]
    pairs += [(b.at[:, r, :], v.at[r]) for b, v in ((col_bank, col_v), (row_bank, row_v)) for r in range(2)]
    pairs += [(volume, volume_v), (measured.at[0], measured_v)]
    copies = [pltpu.make_async_copy(a, b, sems.at[i]) for i, (a, b) in enumerate(pairs)]
    for copy in copies:
        copy.start()
    place = Place(paired)
    planes = volume.shape[0]
    reach = (row_bank.shape[0] - 1) // 2
    for copy in copies[:6]:
        copy.wait()
    pick_taps(view.shape[0], planes, view, index_v[...], (row_v, col_v), taps)
    for d in range(planes):
        column_operands(taps, d, d, reach, (fwd_hi, fwd_lo), None)
    row_hi, row_lo = split(row_operand(taps, 0, planes, reach, place))
    for copy in copies[6:]:
        copy.wait()
    target = window_target(measured_v[...], place) if paired else 0.0
    mine[...], other[...] = forward(
        [volume_v[d] for d in range(planes)], fwd_hi, fwd_lo, row_hi, row_lo, target, w_hi, w_lo
    )


def prepare_kernel(paired, planes, reach, back, ahead, taps, *outs):
    place = Place(paired)
    fwd_hi, fwd_lo, row_hi, row_lo = outs[:4]
    wanted = sorted(set(back) | {ahead})
    for step in wanted:
        adj, adj_rows = outs[4 + 2 * back.index(step) :][:2] if step in back else (None, None)
        for d in range(planes):
            column_operands(
                taps, step * planes + d, d, reach, (fwd_hi, fwd_lo) if step == ahead else None, adj
            )
        stack = row_operand(taps, step, planes, reach, place)
        if step == ahead:
            row_hi[...], row_lo[...] = split(stack)
        if step in back:
            adj_rows[...] = adjoint_row_operand(stack)


def middle_kernel(
    paired, step, kept, crossed, swapped, adj, adj_rows, fwd_hi, fwd_lo, row_hi, row_lo,
    volume, measured, mine, other, fresh, w_hi, w_lo,
):
    place = Place(paired)
    residual = jnp.concatenate(joined(place, kept[...], crossed[...], swapped[...]), axis=0)

    def emit(d, plane):
        fresh[d] = plane

    planes = [volume[d] for d in range(volume.shape[0])]
    planes = adjoint(residual, adj_rows[...], adj, planes, emit)
    target = window_target(measured[step], place) if paired else 0.0
    mine[...], other[...] = forward(
        planes, fwd_hi, fwd_lo, row_hi[...], row_lo[...], target, w_hi, w_lo
    )


def last_kernel(
    paired, kept, crossed, swapped, adj, adj_rows, volume, fresh, residual_out,
    fresh_v, residual_v, sems,
):
    place = Place(paired)
    mine, other = joined(place, kept[...], crossed[...], swapped[...])
    reach = mine.shape[0] // 2
    lower = place.flag == 1
    own = jnp.concatenate(
        [jnp.where(lower, other[reach:], mine[reach:]), jnp.where(lower, mine[:reach], other[:reach])],
        axis=0,
    )
    residual_v[...] = pltpu.roll(own, own.shape[1] - HALF, 1)
    count = volume.shape[0]
    copies = [pltpu.make_async_copy(fresh_v.at[d], fresh.at[d], sems.at[d]) for d in range(count)]
    copies.append(pltpu.make_async_copy(residual_v, residual_out, sems.at[count]))
    copies[count].start()

    def emit(d, plane):
        fresh_v[d] = plane
        copies[d].start()

    planes = [volume[d] for d in range(count)]
    adjoint(jnp.concatenate([mine, other], axis=0), adj_rows[...], adj, planes, emit)
    for copy in copies:
        copy.wait()


VMEM = pl.BlockSpec(memory_space=pltpu.VMEM)
HBM = pl.BlockSpec(memory_space=pltpu.HBM)


def call(kernel, in_specs, out_specs, outs, scratch, flops, name, args):
    return pl.pallas_call(
        kernel,
        out_shape=outs,
        in_specs=in_specs,
        out_specs=out_specs,
        scratch_shapes=scratch,
        compiler_params=pltpu.CompilerParams(vmem_limit_bytes=24 << 20),
        cost_estimate=pl.CostEstimate(flops=flops, bytes_accessed=4 << 20, transcendentals=0),
        name=name,
    )(*args)


def per_device(volume, measured, row_bank, col_bank, kernel_index, view_order):
    planes, rows, width = volume.shape
    steps = measured.shape[0]
    reach = (row_bank.shape[2] - 1) // 2
    assert rows == 2 * reach and width % LANES == 0 and reach <= HALF
    depth, tiles = lax.axis_size("depth"), lax.axis_size("tile")
    d, t = lax.axis_index("depth"), lax.axis_index("tile")
    paired = depth == 2 and tiles % 2 == 0 and tiles > 2
    place = Place(paired)

    def flow(spot):
        side, i = divmod(spot, tiles)
        if i in (0, tiles - 1):
            return i ^ 1 if side else tiles + i
        return tiles + (i + 1 if i % 2 else i - 1) if side else i ^ 1

    def exchange(mine, other, step, during):
        if paired:
            swap = [(0, 1), (1, 0)]
            kept = mine + lax.ppermute(other, "depth", swap)
            crossed = lax.ppermute(
                kept, ("depth", "tile"), [(i, flow(i)) for i in range(2 * tiles)]
            )
            ready = during()
            if ready:
                crossed, *ready = lax.optimization_barrier((crossed, *ready))
            send = jnp.where(place.end_odd, 0.0, kept) + jnp.where(place.end_even, 0.0, crossed)
            return kept, crossed, lax.ppermute(send, "depth", swap), ready
        target = jnp.roll(measured[step], HALF, axis=1)
        high = jnp.pad(target[:reach], ((reach, 0), (0, 0)))
        low = jnp.pad(target[reach:], ((0, reach), (0, 0)))
        lower = place.flag == 1
        evens = [(i, i ^ 1) for i in range(tiles) if i ^ 1 < tiles]
        odds = [(i, i + 1 if i % 2 else i - 1) for i in range(tiles)]
        odds = [(i, j) for i, j in odds if 0 <= j < tiles]
        kept = lax.psum(mine, "depth") - jnp.where(lower, low, high)
        rest = lax.psum(other, "depth") - jnp.where(lower, high, low)
        rest = rest + lax.ppermute(rest, "tile", odds)
        return kept, lax.ppermute(kept, "tile", evens), rest, during()

    shape = jax.ShapeDtypeStruct
    stacks = 2 * planes * rows
    forward_shapes = [
        shape((planes, 2 * LANES, 2 * LANES), bf16),
        shape((planes, 2 * LANES, 2 * LANES), bf16),
        shape((2 * rows, stacks), bf16),
        shape((2 * rows, stacks), bf16),
    ]
    adjoint_shapes = [
        shape((planes, 2, 2 * LANES, 2 * LANES), bf16),
        shape((stacks, 6 * rows), bf16),
    ]
    image = shape((rows, width), f32)
    block = shape(volume.shape, f32)
    lines = -(-steps * planes // 16) * 16
    tap_shape = shape((4, lines, LANES), f32)
    scratch = [pltpu.VMEM((stacks, width), bf16)] * 2
    work = 400 << 20

    index = kernel_index.T
    banks = [jnp.transpose(x, (2, 1, 0)) for x in (row_bank, col_bank)]
    mine, other, taps = call(
        functools.partial(first_kernel, paired), [HBM] * 6, [VMEM] * 3,
        [image, image, tap_shape],
        [pltpu.SMEM(view_order.shape, jnp.int32)]
        + [pltpu.VMEM(index.shape, index.dtype)]
        + [pltpu.VMEM((2, x.shape[0], x.shape[2]), f32) for x in banks]
        + [pltpu.VMEM(x.shape, f32) for x in (volume, measured[0])]
        + [pltpu.VMEM(x.shape, x.dtype) for x in forward_shapes[:2]]
        + scratch + [pltpu.SemaphoreType.DMA((8,))],
        work, "first",
        [pltpu.with_memory_space_constraint(x, pltpu.HBM)
         for x in (view_order, index, *banks, volume, measured)],
    )

    def prepare(back, ahead):
        outs = forward_shapes + adjoint_shapes * len(back)
        return call(
            functools.partial(prepare_kernel, paired, planes, reach, back, ahead),
            [VMEM], [VMEM] * len(outs), outs, [], work, "prepare", (taps,),
        )

    adjoints = []
    for step in range(1, steps):
        back = (0, 1) if step == 1 else (step,)
        kept, crossed, swapped, ready = exchange(
            mine, other, step - 1, lambda: prepare(back, step)
        )
        forwards = ready[:4]
        adjoints += [ready[i : i + 2] for i in range(4, len(ready), 2)]
        mine, other, volume = call(
            functools.partial(middle_kernel, paired, step), [VMEM] * 11, [VMEM] * 3,
            [image, image, block], scratch, 2 * work, "middle",
            (kept, crossed, swapped, *adjoints[step - 1], *forwards, volume, measured),
        )
    kept, crossed, swapped, _ = exchange(mine, other, steps - 1, lambda: [])
    return call(
        functools.partial(last_kernel, paired), [VMEM] * 6, [HBM] * 2, [block, image],
        [pltpu.VMEM(volume.shape, f32), pltpu.VMEM((rows, width), f32),
         pltpu.SemaphoreType.DMA((planes + 1,))],
        work, "last", (kept, crossed, swapped, *adjoints[steps - 1], volume),
    )


def solution(mesh):
    return jax.shard_map(
        per_device,
        mesh=mesh,
        in_specs=(P("depth", "tile", None), P(None, "tile", None), P(), P(), P(None, "depth"), P()),
        out_specs=(P("depth", "tile", None), P("tile", None)),
        check_vma=False,
    )
```

```python
import functools

import jax
import jax.numpy as jnp
from jax import lax
from jax.experimental import pallas as pl
from jax.experimental.pallas import tpu as pltpu
from jax.sharding import PartitionSpec as P

descent_step = 0.5
shrinkage = 0.1
LANES = 128
HALF = LANES // 2
bf16, f32 = jnp.bfloat16, jnp.float32


def split(x):
    hi = x.astype(bf16)
    return hi, (x - hi.astype(f32)).astype(bf16)


def dot(a, b):
    return lax.dot_general(a, b, (((1,), (0,)), ((), ())), preferred_element_type=f32)


def dot_nt(a, b):
    return lax.dot_general(a, b, (((1,), (1,)), ((), ())), preferred_element_type=f32)


def lane_iota(shape):
    return lax.broadcasted_iota(jnp.int32, shape, 1)


def row_iota(shape):
    return lax.broadcasted_iota(jnp.int32, shape, 0)


class Place:
    def __init__(self, paired):
        d, t = lax.axis_index("depth"), lax.axis_index("tile")
        tiles = lax.axis_size("tile")
        odd = lax.rem(t, 2)
        self.first = t == 0
        self.last = t == tiles - 1
        end = jnp.logical_or(self.first, self.last)
        side = jnp.where(end, 1 - d, d)
        self.flag = 1 - jnp.bitwise_xor(odd, side) if paired else 1 - odd
        end = jnp.logical_and(end, paired)
        self.end_even = jnp.logical_and(end, side == 0)
        self.end_odd = jnp.logical_and(end, side == 1)


def pick_taps(steps, planes, view_ref, index, banks, taps_ref):
    count = taps_ref.shape[1]
    index = index.astype(f32)
    copies = jnp.concatenate([index] * (count // planes), axis=0)
    line, lane = row_iota(copies.shape), lane_iota(copies.shape)
    view = jnp.full(copies.shape, view_ref[0], jnp.int32)
    for step in range(1, steps):
        view = jnp.where(line >= step * planes, view_ref[step], view)
    entry = jnp.sum(jnp.where(lane == view, copies, 0.0), axis=1, keepdims=True)
    size = banks[0].shape[2]
    chosen = (lane_iota((count, size)).astype(f32) == entry).astype(f32).astype(bf16)
    taps_ref[...] = jnp.zeros(taps_ref.shape, f32)
    for b, bank in enumerate(banks):
        for r in range(2):
            hi, lo = split(bank[r])
            taps = dot_nt(chosen, hi) + dot_nt(chosen, lo)
            taps_ref[2 * b + r, :, 0 : taps.shape[1]] = taps


def column_operands(taps_ref, line, d, reach, forward_out, adjoint_out):
    square = (LANES, LANES)
    below = (lane_iota(square) < row_iota(square)).astype(f32).astype(bf16)
    above = (lane_iota(square) > row_iota(square)).astype(f32).astype(bf16)
    for r in range(2):
        base = pltpu.roll(
            jnp.broadcast_to(taps_ref[2 + r, line : line + 1], (8, LANES)),
            (LANES - HALF - reach) % LANES, 1, stride=1, stride_axis=0,
        )
        ring = jnp.concatenate(
            [base] + [pltpu.roll(base, 8 * b, 1) for b in range(1, LANES // 8)], axis=0
        )
        hi, lo = split(ring)
        low_hi, low_lo, up_hi, up_lo = hi * below, lo * below, hi * above, lo * above
        left, right = slice(0, LANES), slice(LANES, 2 * LANES)
        if forward_out is not None:
            fwd_hi, fwd_lo = forward_out
            here = slice(r * LANES, (r + 1) * LANES)
            fwd_hi[d, here, left] = up_hi
            fwd_hi[d, here, right] = low_hi
            fwd_lo[d, here, left] = up_lo
            fwd_lo[d, here, right] = low_lo
        if adjoint_out is not None:
            adjoint_out[d, r, left, left] = low_hi
            adjoint_out[d, r, left, right] = low_lo
            adjoint_out[d, r, right, left] = up_hi
            adjoint_out[d, r, right, right] = up_lo


def row_operand(taps_ref, step, planes, reach, place):
    rows = 2 * reach
    per_lane = LANES // rows
    window, lane = row_iota((8, LANES)), lane_iota((8, LANES)) // rows
    parts = []
    for k in range(2 * planes):
        line = step * planes + k // 2
        parts.append(
            pltpu.roll(
                jnp.broadcast_to(taps_ref[k % 2, line : line + 1], (8, LANES)),
                ((k % per_lane) * rows - 2 * reach) % LANES, 1, stride=1, stride_axis=0,
            )
        )
    bands = []
    for band in range(2 * rows // 8):
        start = (8 * band) % rows
        offset = start + rows * (place.flag if band < rows // 8 else 1 - place.flag)
        spot = window + offset
        good = jnp.logical_and(
            jnp.logical_or(jnp.logical_not(place.first), spot >= reach),
            jnp.logical_or(jnp.logical_not(place.last), spot < rows + reach),
        )
        line = []
        for group in range(2 * planes // per_lane):
            total = jnp.zeros((8, LANES), f32)
            for k in range(per_lane):
                part = pltpu.roll(parts[group * per_lane + k], offset, 1)
                total = jnp.where(lane == k, part, total)
            line.append(jnp.where(good, total, 0.0))
        bands.append(jnp.concatenate(line, axis=1))
    return jnp.concatenate(bands, axis=0)


def adjoint_row_operand(stack):
    hi, lo = split(stack.T)
    return jnp.concatenate([hi, hi, lo], axis=1)


def forward(volume, fwd_hi, fwd_lo, row_hi, row_lo, w_hi, w_lo):
    planes = len(volume)
    rows, width = volume[0].shape
    blocks = width // LANES
    zero = jnp.zeros((rows, LANES), bf16)
    left = lane_iota((rows, LANES)) < HALF
    for d in range(planes):
        sides = []
        for part in split(volume[d]):
            column = [zero] + [part[:, b * LANES : (b + 1) * LANES] for b in range(blocks)] + [zero]
            column = jnp.concatenate(column, axis=0)
            sides.append(jnp.concatenate([column[:-rows], column[rows:]], axis=1))
        hi, lo = sides
        wide = dot_nt(hi, fwd_hi[d]) + dot_nt(lo, fwd_hi[d]) + dot_nt(hi, fwd_lo[d])
        for r in range(2):
            part = wide[:, r * LANES : (r + 1) * LANES]
            spot = pl.ds((2 * d + r) * rows, rows)
            for c in range(blocks):
                block = part[c * rows : (c + 1) * rows]
                if c == 0:
                    block = jnp.where(left, part[blocks * rows :], block)
                hi_w, lo_w = split(block)
                w_hi[spot, c * LANES : (c + 1) * LANES] = hi_w
                w_lo[spot, c * LANES : (c + 1) * LANES] = lo_w
    return row_pass(row_hi[rows:], row_lo[rows:], w_hi, w_lo)


def row_pass(row_hi, row_lo, w_hi, w_lo):
    return dot(row_hi, w_hi[...]) + dot(row_lo, w_hi[...]) + dot(row_hi, w_lo[...])


def adjoint(residual, adj_rows, adj, volume, emit):
    planes = len(volume)
    rows, width = volume[0].shape
    blocks = width // LANES
    hi, lo = split(residual)
    upper = dot(adj_rows, jnp.concatenate([hi, lo, hi], axis=0))
    left = lane_iota((rows, LANES)) < HALF
    result = []

    def product(d):
        total = None
        for r in range(2):
            spot = (2 * d + r) * rows
            part = upper[spot : spot + rows]
            edge = part[:, :LANES]
            column = [jnp.where(left, 0.0, edge)]
            column += [part[:, b * LANES : (b + 1) * LANES] for b in range(1, blocks)]
            column += [jnp.where(left, edge, 0.0)]
            for side in split(jnp.concatenate(column, axis=0)):
                side = jnp.concatenate([side[:-rows], side[rows:]], axis=1)
                term = dot(side, adj[d, r])
                total = term if total is None else total + term
        return total

    ahead = product(0)
    for d in range(planes):
        total, ahead = ahead, product(d + 1) if d + 1 < planes else None
        grad = total[:, :LANES] + total[:, LANES:]
        grad = jnp.concatenate([grad[c * rows : (c + 1) * rows] for c in range(blocks)], axis=1)
        moved = volume[d] - descent_step * grad
        plane = moved - jnp.clip(moved, -shrinkage, shrinkage)
        emit(d, plane)
        result.append(plane)
    return result


def window_target(measured, place):
    reach = measured.shape[0] // 2
    upper = jnp.where(place.flag == 1, measured[reach:], 0.0)
    lower = jnp.where(place.flag == 1, 0.0, measured[:reach])
    return pltpu.roll(jnp.concatenate([upper, lower], axis=0), HALF, 1)


def joined(place, kept, crossed, swapped):
    add = jnp.where(place.end_even, swapped, jnp.where(place.end_odd, 0.0, crossed))
    other = jnp.where(
        place.end_even, crossed, jnp.where(place.end_odd, crossed + swapped, swapped)
    )
    return kept + add, other


def first_kernel(
    paired, view_h, index, row_bank, col_bank, volume, measured,
    other, taps, measured_v, row_hi, row_lo, w_hi, w_lo,
    view, index_v, row_v, col_v, volume_v, fwd_hi, fwd_lo, sems,
):
    pairs = [(view_h, view), (index, index_v)]
    pairs += [(b.at[:, r, :], v.at[r]) for b, v in ((col_bank, col_v), (row_bank, row_v)) for r in range(2)]
    pairs += [(volume, volume_v), (measured.at[0], measured_v.at[0])]
    copies = [pltpu.make_async_copy(a, b, sems.at[i]) for i, (a, b) in enumerate(pairs)]
    for copy in copies:
        copy.start()
    place = Place(paired)
    planes = volume.shape[0]
    reach = (row_bank.shape[0] - 1) // 2
    for copy in copies[:6]:
        copy.wait()
    pick_taps(view.shape[0], planes, view, index_v[...], (row_v, col_v), taps)
    for d in range(planes):
        column_operands(taps, d, d, reach, (fwd_hi, fwd_lo), None)
    hi, lo = split(row_operand(taps, 0, planes, reach, place))
    row_hi[...], row_lo[...] = hi, lo
    for copy in copies[6:]:
        copy.wait()
    other[...] = forward(
        [volume_v[d] for d in range(planes)], fwd_hi, fwd_lo, hi, lo, w_hi, w_lo
    )


def keep_kernel(paired, step, measured, row_hi, row_lo, w_hi, w_lo, mine):
    rows = mine.shape[0]
    image = row_pass(row_hi[:rows], row_lo[:rows], w_hi, w_lo)
    if paired:
        image = image - window_target(measured[step], Place(paired))
    mine[...] = image


def prepare_kernel(paired, planes, reach, back, ahead, taps, *outs):
    place = Place(paired)
    fwd_hi, fwd_lo, row_hi, row_lo = outs[:4]
    wanted = sorted(set(back) | {ahead})
    for step in wanted:
        adj, adj_rows = outs[4 + 2 * back.index(step) :][:2] if step in back else (None, None)
        for d in range(planes):
            column_operands(
                taps, step * planes + d, d, reach, (fwd_hi, fwd_lo) if step == ahead else None, adj
            )
        stack = row_operand(taps, step, planes, reach, place)
        if step == ahead:
            row_hi[...], row_lo[...] = split(stack)
        if step in back:
            adj_rows[...] = adjoint_row_operand(stack)


def middle_kernel(
    paired, kept, crossed, swapped, adj, adj_rows, fwd_hi, fwd_lo, row_hi, row_lo, volume,
    other, fresh, w_hi, w_lo,
):
    place = Place(paired)
    residual = jnp.concatenate(joined(place, kept[...], crossed[...], swapped[...]), axis=0)

    def emit(d, plane):
        fresh[d] = plane

    planes = [volume[d] for d in range(volume.shape[0])]
    planes = adjoint(residual, adj_rows[...], adj, planes, emit)
    other[...] = forward(planes, fwd_hi, fwd_lo, row_hi[...], row_lo[...], w_hi, w_lo)


def last_kernel(
    paired, kept, crossed, swapped, adj, adj_rows, volume, fresh, residual_out,
    fresh_v, residual_v, sems,
):
    place = Place(paired)
    mine, other = joined(place, kept[...], crossed[...], swapped[...])
    reach = mine.shape[0] // 2
    lower = place.flag == 1
    own = jnp.concatenate(
        [jnp.where(lower, other[reach:], mine[reach:]), jnp.where(lower, mine[:reach], other[:reach])],
        axis=0,
    )
    residual_v[...] = pltpu.roll(own, own.shape[1] - HALF, 1)
    count = volume.shape[0]
    copies = [pltpu.make_async_copy(fresh_v.at[d], fresh.at[d], sems.at[d]) for d in range(count)]
    copies.append(pltpu.make_async_copy(residual_v, residual_out, sems.at[count]))
    copies[count].start()

    def emit(d, plane):
        fresh_v[d] = plane
        copies[d].start()

    planes = [volume[d] for d in range(count)]
    adjoint(jnp.concatenate([mine, other], axis=0), adj_rows[...], adj, planes, emit)
    for copy in copies:
        copy.wait()


VMEM = pl.BlockSpec(memory_space=pltpu.VMEM)
HBM = pl.BlockSpec(memory_space=pltpu.HBM)


def call(kernel, in_specs, out_specs, outs, scratch, flops, name, args):
    return pl.pallas_call(
        kernel,
        out_shape=outs,
        in_specs=in_specs,
        out_specs=out_specs,
        scratch_shapes=scratch,
        compiler_params=pltpu.CompilerParams(vmem_limit_bytes=24 << 20),
        cost_estimate=pl.CostEstimate(flops=flops, bytes_accessed=4 << 20, transcendentals=0),
        name=name,
    )(*args)


def per_device(volume, measured, row_bank, col_bank, kernel_index, view_order):
    planes, rows, width = volume.shape
    steps = measured.shape[0]
    reach = (row_bank.shape[2] - 1) // 2
    assert rows == 2 * reach and width % LANES == 0 and reach <= HALF
    depth, tiles = lax.axis_size("depth"), lax.axis_size("tile")
    d, t = lax.axis_index("depth"), lax.axis_index("tile")
    paired = depth == 2 and tiles % 2 == 0 and tiles > 2
    place = Place(paired)

    def flow(spot):
        side, i = divmod(spot, tiles)
        if i in (0, tiles - 1):
            return i ^ 1 if side else tiles + i
        return tiles + (i + 1 if i % 2 else i - 1) if side else i ^ 1

    def exchange(keep, other, step, during):
        if paired:
            swap = [(0, 1), (1, 0)]
            kept = sum(lax.optimization_barrier((keep(), lax.ppermute(other, "depth", swap))))
            crossed = lax.ppermute(
                kept, ("depth", "tile"), [(i, flow(i)) for i in range(2 * tiles)]
            )
            ready = during()
            if ready:
                crossed, *ready = lax.optimization_barrier((crossed, *ready))
            send = jnp.where(place.end_odd, 0.0, kept) + jnp.where(place.end_even, 0.0, crossed)
            return kept, crossed, lax.ppermute(send, "depth", swap), ready
        target = jnp.roll(measured[step], HALF, axis=1)
        high = jnp.pad(target[:reach], ((reach, 0), (0, 0)))
        low = jnp.pad(target[reach:], ((0, reach), (0, 0)))
        lower = place.flag == 1
        evens = [(i, i ^ 1) for i in range(tiles) if i ^ 1 < tiles]
        odds = [(i, i + 1 if i % 2 else i - 1) for i in range(tiles)]
        odds = [(i, j) for i, j in odds if 0 <= j < tiles]
        kept = lax.psum(keep(), "depth") - jnp.where(lower, low, high)
        rest = lax.psum(other, "depth") - jnp.where(lower, high, low)
        rest = rest + lax.ppermute(rest, "tile", odds)
        return kept, lax.ppermute(kept, "tile", evens), rest, during()

    shape = jax.ShapeDtypeStruct
    stacks = 2 * planes * rows
    forward_shapes = [
        shape((planes, 2 * LANES, 2 * LANES), bf16),
        shape((planes, 2 * LANES, 2 * LANES), bf16),
        shape((2 * rows, stacks), bf16),
        shape((2 * rows, stacks), bf16),
    ]
    adjoint_shapes = [
        shape((planes, 2, 2 * LANES, 2 * LANES), bf16),
        shape((stacks, 6 * rows), bf16),
    ]
    image = shape((rows, width), f32)
    block = shape(volume.shape, f32)
    lines = -(-steps * planes // 16) * 16
    tap_shape = shape((4, lines, LANES), f32)
    columns = [shape((stacks, width), bf16)] * 2
    work = 400 << 20

    index = kernel_index.T
    banks = [jnp.transpose(x, (2, 1, 0)) for x in (row_bank, col_bank)]
    outs = [image, tap_shape, shape((1, rows, width), f32), *forward_shapes[2:], *columns]
    other, taps, target, row_hi, row_lo, *wide = call(
        functools.partial(first_kernel, paired), [HBM] * 6, [VMEM] * len(outs), outs,
        [pltpu.SMEM(view_order.shape, jnp.int32)]
        + [pltpu.VMEM(index.shape, index.dtype)]
        + [pltpu.VMEM((2, x.shape[0], x.shape[2]), f32) for x in banks]
        + [pltpu.VMEM(x.shape, x.dtype) for x in (volume, *forward_shapes[:2])]
        + [pltpu.SemaphoreType.DMA((8,))],
        work, "first",
        [pltpu.with_memory_space_constraint(x, pltpu.HBM)
         for x in (view_order, index, *banks, volume, measured)],
    )

    def keeper(step, *args):
        return lambda: call(
            functools.partial(keep_kernel, paired, step), [VMEM] * 5, [VMEM], [image], [],
            work // 10, "keep", args,
        )[0]

    keep = keeper(0, target, row_hi, row_lo, *wide)

    def prepare(back, ahead):
        outs = forward_shapes + adjoint_shapes * len(back)
        return call(
            functools.partial(prepare_kernel, paired, planes, reach, back, ahead),
            [VMEM], [VMEM] * len(outs), outs, [], work, "prepare", (taps,),
        )

    adjoints = []
    for step in range(1, steps):
        back = (0, 1) if step == 1 else (step,)
        kept, crossed, swapped, ready = exchange(
            keep, other, step - 1, lambda: prepare(back, step)
        )
        forwards = ready[:4]
        adjoints += [ready[i : i + 2] for i in range(4, len(ready), 2)]
        outs = [image, block, *columns]
        other, volume, *wide = call(
            functools.partial(middle_kernel, paired), [VMEM] * 10, [VMEM] * 4, outs, [],
            2 * work, "middle",
            (kept, crossed, swapped, *adjoints[step - 1], *forwards, volume),
        )
        keep = keeper(step, measured, *forwards[2:], *wide)
    kept, crossed, swapped, _ = exchange(keep, other, steps - 1, lambda: [])
    return call(
        functools.partial(last_kernel, paired), [VMEM] * 6, [HBM] * 2, [block, image],
        [pltpu.VMEM(volume.shape, f32), pltpu.VMEM((rows, width), f32),
         pltpu.SemaphoreType.DMA((planes + 1,))],
        work, "last", (kept, crossed, swapped, *adjoints[steps - 1], volume),
    )


def solution(mesh):
    return jax.shard_map(
        per_device,
        mesh=mesh,
        in_specs=(P("depth", "tile", None), P(None, "tile", None), P(), P(), P(None, "depth"), P()),
        out_specs=(P("depth", "tile", None), P("tile", None)),
        check_vma=False,
    )
```

```python
import functools

import jax
import jax.numpy as jnp
from jax import lax
from jax.experimental import pallas as pl
from jax.experimental.pallas import tpu as pltpu
from jax.sharding import PartitionSpec as P

descent_step = 0.5
shrinkage = 0.1
LANES = 128
HALF = LANES // 2
bf16, f32 = jnp.bfloat16, jnp.float32


def split(x):
    hi = x.astype(bf16)
    return hi, (x - hi.astype(f32)).astype(bf16)


def dot(a, b):
    return lax.dot_general(a, b, (((1,), (0,)), ((), ())), preferred_element_type=f32)


def dot_nt(a, b):
    return lax.dot_general(a, b, (((1,), (1,)), ((), ())), preferred_element_type=f32)


def lane_iota(shape):
    return lax.broadcasted_iota(jnp.int32, shape, 1)


def row_iota(shape):
    return lax.broadcasted_iota(jnp.int32, shape, 0)


class Place:
    def __init__(self, paired):
        d, t = lax.axis_index("depth"), lax.axis_index("tile")
        tiles = lax.axis_size("tile")
        odd = lax.rem(t, 2)
        self.first = t == 0
        self.last = t == tiles - 1
        end = jnp.logical_or(self.first, self.last)
        side = jnp.where(end, 1 - d, d)
        self.flag = 1 - jnp.bitwise_xor(odd, side) if paired else 1 - odd
        end = jnp.logical_and(end, paired)
        self.end_even = jnp.logical_and(end, side == 0)
        self.end_odd = jnp.logical_and(end, side == 1)


def pick_taps(steps, planes, view_ref, index, banks, taps_ref):
    count = taps_ref.shape[1]
    index = index.astype(f32)
    copies = jnp.concatenate([index] * (count // planes), axis=0)
    line, lane = row_iota(copies.shape), lane_iota(copies.shape)
    view = jnp.full(copies.shape, view_ref[0], jnp.int32)
    for step in range(1, steps):
        view = jnp.where(line >= step * planes, view_ref[step], view)
    entry = jnp.sum(jnp.where(lane == view, copies, 0.0), axis=1, keepdims=True)
    size = banks[0].shape[2]
    chosen = (lane_iota((count, size)).astype(f32) == entry).astype(f32).astype(bf16)
    taps_ref[...] = jnp.zeros(taps_ref.shape, f32)
    for b, bank in enumerate(banks):
        for r in range(2):
            hi, lo = split(bank[r])
            taps = dot_nt(chosen, hi) + dot_nt(chosen, lo)
            taps_ref[2 * b + r, :, 0 : taps.shape[1]] = taps


def column_operands(taps_ref, line, d, reach, forward_out, adjoint_out):
    square = (LANES, LANES)
    below = (lane_iota(square) < row_iota(square)).astype(f32).astype(bf16)
    above = (lane_iota(square) > row_iota(square)).astype(f32).astype(bf16)
    for r in range(2):
        base = pltpu.roll(
            jnp.broadcast_to(taps_ref[2 + r, line : line + 1], (8, LANES)),
            (LANES - HALF - reach) % LANES, 1, stride=1, stride_axis=0,
        )
        ring = jnp.concatenate(
            [base] + [pltpu.roll(base, 8 * b, 1) for b in range(1, LANES // 8)], axis=0
        )
        hi, lo = split(ring)
        low_hi, low_lo, up_hi, up_lo = hi * below, lo * below, hi * above, lo * above
        left, right = slice(0, LANES), slice(LANES, 2 * LANES)
        if forward_out is not None:
            fwd_hi, fwd_lo = forward_out
            here = slice(r * LANES, (r + 1) * LANES)
            fwd_hi[d, here, left] = up_hi
            fwd_hi[d, here, right] = low_hi
            fwd_lo[d, here, left] = up_lo
            fwd_lo[d, here, right] = low_lo
        if adjoint_out is not None:
            adjoint_out[d, r, left, left] = low_hi
            adjoint_out[d, r, left, right] = low_lo
            adjoint_out[d, r, right, left] = up_hi
            adjoint_out[d, r, right, right] = up_lo


def row_operand(taps_ref, step, planes, reach, place):
    rows = 2 * reach
    per_lane = LANES // rows
    window, lane = row_iota((8, LANES)), lane_iota((8, LANES)) // rows
    parts = []
    for k in range(2 * planes):
        line = step * planes + k // 2
        parts.append(
            pltpu.roll(
                jnp.broadcast_to(taps_ref[k % 2, line : line + 1], (8, LANES)),
                ((k % per_lane) * rows - 2 * reach) % LANES, 1, stride=1, stride_axis=0,
            )
        )
    bands = []
    for band in range(2 * rows // 8):
        start = (8 * band) % rows
        offset = start + rows * (place.flag if band < rows // 8 else 1 - place.flag)
        spot = window + offset
        good = jnp.logical_and(
            jnp.logical_or(jnp.logical_not(place.first), spot >= reach),
            jnp.logical_or(jnp.logical_not(place.last), spot < rows + reach),
        )
        line = []
        for group in range(2 * planes // per_lane):
            total = jnp.zeros((8, LANES), f32)
            for k in range(per_lane):
                part = pltpu.roll(parts[group * per_lane + k], offset, 1)
                total = jnp.where(lane == k, part, total)
            line.append(jnp.where(good, total, 0.0))
        bands.append(jnp.concatenate(line, axis=1))
    return jnp.concatenate(bands, axis=0)


def adjoint_row_operand(stack):
    hi, lo = split(stack.T)
    return jnp.concatenate([hi, hi, lo], axis=1)


def forward(volume, fwd_hi, fwd_lo, row_hi, row_lo, w_hi, w_lo):
    planes = len(volume)
    rows, width = volume[0].shape
    blocks = width // LANES
    zero = jnp.zeros((rows, LANES), bf16)
    left = lane_iota((rows, LANES)) < HALF
    for d in range(planes):
        sides = []
        for part in split(volume[d]):
            column = [zero] + [part[:, b * LANES : (b + 1) * LANES] for b in range(blocks)] + [zero]
            column = jnp.concatenate(column, axis=0)
            sides.append(jnp.concatenate([column[:-rows], column[rows:]], axis=1))
        hi, lo = sides
        wide = dot_nt(hi, fwd_hi[d]) + dot_nt(lo, fwd_hi[d]) + dot_nt(hi, fwd_lo[d])
        for r in range(2):
            part = wide[:, r * LANES : (r + 1) * LANES]
            spot = pl.ds((2 * d + r) * rows, rows)
            for c in range(blocks):
                block = part[c * rows : (c + 1) * rows]
                if c == 0:
                    block = jnp.where(left, part[blocks * rows :], block)
                hi_w, lo_w = split(block)
                w_hi[spot, c * LANES : (c + 1) * LANES] = hi_w
                w_lo[spot, c * LANES : (c + 1) * LANES] = lo_w
    return row_pass(row_hi[rows:], row_lo[rows:], w_hi, w_lo)


def row_pass(row_hi, row_lo, w_hi, w_lo):
    return dot(row_hi, w_hi[...]) + dot(row_lo, w_hi[...]) + dot(row_hi, w_lo[...])


def adjoint(residual, adj_rows, adj, volume, emit):
    planes = len(volume)
    rows, width = volume[0].shape
    blocks = width // LANES
    hi, lo = split(residual)
    upper = dot(adj_rows, jnp.concatenate([hi, lo, hi], axis=0))
    left = lane_iota((rows, LANES)) < HALF
    result = []

    def product(d):
        total = None
        for r in range(2):
            spot = (2 * d + r) * rows
            part = upper[spot : spot + rows]
            edge = part[:, :LANES]
            column = [jnp.where(left, 0.0, edge)]
            column += [part[:, b * LANES : (b + 1) * LANES] for b in range(1, blocks)]
            column += [jnp.where(left, edge, 0.0)]
            for side in split(jnp.concatenate(column, axis=0)):
                side = jnp.concatenate([side[:-rows], side[rows:]], axis=1)
                term = dot(side, adj[d, r])
                total = term if total is None else total + term
        return total

    ahead = product(0)
    for d in range(planes):
        total, ahead = ahead, product(d + 1) if d + 1 < planes else None
        grad = total[:, :LANES] + total[:, LANES:]
        grad = jnp.concatenate([grad[c * rows : (c + 1) * rows] for c in range(blocks)], axis=1)
        moved = volume[d] - descent_step * grad
        plane = moved - jnp.clip(moved, -shrinkage, shrinkage)
        emit(d, plane)
        result.append(plane)
    return result


def window_target(measured, place):
    reach = measured.shape[0] // 2
    upper = jnp.where(place.flag == 1, measured[reach:], 0.0)
    lower = jnp.where(place.flag == 1, 0.0, measured[:reach])
    return pltpu.roll(jnp.concatenate([upper, lower], axis=0), HALF, 1)


def joined(place, kept, crossed, swapped):
    add = jnp.where(place.end_even, swapped, jnp.where(place.end_odd, 0.0, crossed))
    other = jnp.where(
        place.end_even, crossed, jnp.where(place.end_odd, crossed + swapped, swapped)
    )
    return kept + add, other


def first_kernel(
    paired, view_h, index, row_bank, col_bank, volume, measured,
    other, taps, measured_v, row_hi, row_lo, w_hi, w_lo,
    view, index_v, row_v, col_v, volume_v, fwd_hi, fwd_lo, sems,
):
    pairs = [(view_h, view), (index, index_v)]
    pairs += [(b.at[:, r, :], v.at[r]) for b, v in ((col_bank, col_v), (row_bank, row_v)) for r in range(2)]
    pairs += [(volume, volume_v), (measured.at[0], measured_v.at[0])]
    copies = [pltpu.make_async_copy(a, b, sems.at[i]) for i, (a, b) in enumerate(pairs)]
    for copy in copies:
        copy.start()
    place = Place(paired)
    planes = volume.shape[0]
    reach = (row_bank.shape[0] - 1) // 2
    for copy in copies[:6]:
        copy.wait()
    pick_taps(view.shape[0], planes, view, index_v[...], (row_v, col_v), taps)
    for d in range(planes):
        column_operands(taps, d, d, reach, (fwd_hi, fwd_lo), None)
    hi, lo = split(row_operand(taps, 0, planes, reach, place))
    row_hi[...], row_lo[...] = hi, lo
    for copy in copies[6:]:
        copy.wait()
    other[...] = forward(
        [volume_v[d] for d in range(planes)], fwd_hi, fwd_lo, hi, lo, w_hi, w_lo
    )


def keep_kernel(paired, step, measured, row_hi, row_lo, w_hi, w_lo, mine):
    rows = mine.shape[0]
    image = row_pass(row_hi[:rows], row_lo[:rows], w_hi, w_lo)
    if paired:
        image = image - window_target(measured[step], Place(paired))
    mine[...] = image


def prepare_kernel(paired, planes, reach, back, ahead, taps, *outs):
    place = Place(paired)
    fwd_hi, fwd_lo, row_hi, row_lo = outs[:4]
    wanted = sorted(set(back) | {ahead})
    for step in wanted:
        adj, adj_rows = outs[4 + 2 * back.index(step) :][:2] if step in back else (None, None)
        for d in range(planes):
            column_operands(
                taps, step * planes + d, d, reach, (fwd_hi, fwd_lo) if step == ahead else None, adj
            )
        stack = row_operand(taps, step, planes, reach, place)
        if step == ahead:
            row_hi[...], row_lo[...] = split(stack)
        if step in back:
            adj_rows[...] = adjoint_row_operand(stack)


def middle_kernel(
    paired, kept, crossed, swapped, adj, adj_rows, fwd_hi, fwd_lo, row_hi, row_lo, volume,
    other, fresh, w_hi, w_lo,
):
    place = Place(paired)
    residual = jnp.concatenate(joined(place, kept[...], crossed[...], swapped[...]), axis=0)

    def emit(d, plane):
        fresh[d] = plane

    planes = [volume[d] for d in range(volume.shape[0])]
    planes = adjoint(residual, adj_rows[...], adj, planes, emit)
    other[...] = forward(planes, fwd_hi, fwd_lo, row_hi[...], row_lo[...], w_hi, w_lo)


def last_kernel(
    paired, kept, crossed, swapped, adj, adj_rows, volume, fresh, residual_out,
    fresh_v, residual_v, sems,
):
    place = Place(paired)
    mine, other = joined(place, kept[...], crossed[...], swapped[...])
    reach = mine.shape[0] // 2
    lower = place.flag == 1
    own = jnp.concatenate(
        [jnp.where(lower, other[reach:], mine[reach:]), jnp.where(lower, mine[:reach], other[:reach])],
        axis=0,
    )
    count = volume.shape[0]
    copies = [pltpu.make_async_copy(fresh_v.at[d], fresh.at[d], sems.at[d]) for d in range(count)]
    copies.append(pltpu.make_async_copy(residual_v, residual_out, sems.at[count]))

    def emit(d, plane):
        fresh_v[d] = plane
        copies[d].start()
        if d == 0:
            residual_v[...] = pltpu.roll(own, own.shape[1] - HALF, 1)
            copies[count].start()

    planes = [volume[d] for d in range(count)]
    adjoint(jnp.concatenate([mine, other], axis=0), adj_rows[...], adj, planes, emit)
    for copy in copies:
        copy.wait()


VMEM = pl.BlockSpec(memory_space=pltpu.VMEM)
HBM = pl.BlockSpec(memory_space=pltpu.HBM)


def call(kernel, in_specs, out_specs, outs, scratch, flops, name, args):
    return pl.pallas_call(
        kernel,
        out_shape=outs,
        in_specs=in_specs,
        out_specs=out_specs,
        scratch_shapes=scratch,
        compiler_params=pltpu.CompilerParams(vmem_limit_bytes=24 << 20),
        cost_estimate=pl.CostEstimate(flops=flops, bytes_accessed=4 << 20, transcendentals=0),
        name=name,
    )(*args)


def per_device(volume, measured, row_bank, col_bank, kernel_index, view_order):
    planes, rows, width = volume.shape
    steps = measured.shape[0]
    reach = (row_bank.shape[2] - 1) // 2
    assert rows == 2 * reach and width % LANES == 0 and reach <= HALF
    depth, tiles = lax.axis_size("depth"), lax.axis_size("tile")
    d, t = lax.axis_index("depth"), lax.axis_index("tile")
    paired = depth == 2 and tiles % 2 == 0 and tiles > 2
    place = Place(paired)

    def flow(spot):
        side, i = divmod(spot, tiles)
        if i in (0, tiles - 1):
            return i ^ 1 if side else tiles + i
        return tiles + (i + 1 if i % 2 else i - 1) if side else i ^ 1

    def exchange(keep, other, step, during):
        if paired:
            swap = [(0, 1), (1, 0)]
            kept = sum(lax.optimization_barrier((keep(), lax.ppermute(other, "depth", swap))))
            crossed = lax.ppermute(
                kept, ("depth", "tile"), [(i, flow(i)) for i in range(2 * tiles)]
            )
            ready = during()
            if ready:
                crossed, *ready = lax.optimization_barrier((crossed, *ready))
            send = jnp.where(place.end_odd, 0.0, kept) + jnp.where(place.end_even, 0.0, crossed)
            return kept, crossed, lax.ppermute(send, "depth", swap), ready
        target = jnp.roll(measured[step], HALF, axis=1)
        high = jnp.pad(target[:reach], ((reach, 0), (0, 0)))
        low = jnp.pad(target[reach:], ((0, reach), (0, 0)))
        lower = place.flag == 1
        evens = [(i, i ^ 1) for i in range(tiles) if i ^ 1 < tiles]
        odds = [(i, i + 1 if i % 2 else i - 1) for i in range(tiles)]
        odds = [(i, j) for i, j in odds if 0 <= j < tiles]
        kept = lax.psum(keep(), "depth") - jnp.where(lower, low, high)
        rest = lax.psum(other, "depth") - jnp.where(lower, high, low)
        rest = rest + lax.ppermute(rest, "tile", odds)
        return kept, lax.ppermute(kept, "tile", evens), rest, during()

    shape = jax.ShapeDtypeStruct
    stacks = 2 * planes * rows
    forward_shapes = [
        shape((planes, 2 * LANES, 2 * LANES), bf16),
        shape((planes, 2 * LANES, 2 * LANES), bf16),
        shape((2 * rows, stacks), bf16),
        shape((2 * rows, stacks), bf16),
    ]
    adjoint_shapes = [
        shape((planes, 2, 2 * LANES, 2 * LANES), bf16),
        shape((stacks, 6 * rows), bf16),
    ]
    image = shape((rows, width), f32)
    block = shape(volume.shape, f32)
    lines = -(-steps * planes // 16) * 16
    tap_shape = shape((4, lines, LANES), f32)
    columns = [shape((stacks, width), bf16)] * 2
    work = 400 << 20

    index = kernel_index.T
    banks = [jnp.transpose(x, (2, 1, 0)) for x in (row_bank, col_bank)]
    outs = [image, tap_shape, shape((1, rows, width), f32), *forward_shapes[2:], *columns]
    other, taps, target, row_hi, row_lo, *wide = call(
        functools.partial(first_kernel, paired), [HBM] * 6, [VMEM] * len(outs), outs,
        [pltpu.SMEM(view_order.shape, jnp.int32)]
        + [pltpu.VMEM(index.shape, index.dtype)]
        + [pltpu.VMEM((2, x.shape[0], x.shape[2]), f32) for x in banks]
        + [pltpu.VMEM(x.shape, x.dtype) for x in (volume, *forward_shapes[:2])]
        + [pltpu.SemaphoreType.DMA((8,))],
        work, "first",
        [pltpu.with_memory_space_constraint(x, pltpu.HBM)
         for x in (view_order, index, *banks, volume, measured)],
    )

    def keeper(step, *args):
        return lambda: call(
            functools.partial(keep_kernel, paired, step), [VMEM] * 5, [VMEM], [image], [],
            work // 10, "keep", args,
        )[0]

    keep = keeper(0, target, row_hi, row_lo, *wide)

    def prepare(back, ahead):
        outs = forward_shapes + adjoint_shapes * len(back)
        return call(
            functools.partial(prepare_kernel, paired, planes, reach, back, ahead),
            [VMEM], [VMEM] * len(outs), outs, [], work, "prepare", (taps,),
        )

    adjoints = []
    for step in range(1, steps):
        back = (0, 1) if step == 1 else (step,)
        kept, crossed, swapped, ready = exchange(
            keep, other, step - 1, lambda: prepare(back, step)
        )
        forwards = ready[:4]
        adjoints += [ready[i : i + 2] for i in range(4, len(ready), 2)]
        outs = [image, block, *columns]
        other, volume, *wide = call(
            functools.partial(middle_kernel, paired), [VMEM] * 10, [VMEM] * 4, outs, [],
            2 * work, "middle",
            (kept, crossed, swapped, *adjoints[step - 1], *forwards, volume),
        )
        keep = keeper(step, measured, *forwards[2:], *wide)
    kept, crossed, swapped, _ = exchange(keep, other, steps - 1, lambda: [])
    return call(
        functools.partial(last_kernel, paired), [VMEM] * 6, [HBM] * 2, [block, image],
        [pltpu.VMEM(volume.shape, f32), pltpu.VMEM((rows, width), f32),
         pltpu.SemaphoreType.DMA((planes + 1,))],
        work, "last", (kept, crossed, swapped, *adjoints[steps - 1], volume),
    )


def solution(mesh):
    return jax.shard_map(
        per_device,
        mesh=mesh,
        in_specs=(P("depth", "tile", None), P(None, "tile", None), P(), P(), P(None, "depth"), P()),
        out_specs=(P("depth", "tile", None), P("tile", None)),
        check_vma=False,
    )
```
